32 devices in a mesh: dp: 32 (over z, y, x, core).
Axes of the slice: x: 2, y: 2, z: 4, core: 2. Of those that a mesh axis runs over, the one named last changes fastest.
Arguments:
- tokens: bfloat16 [65536, 768], P('dp'), may hold values from -6 to 6
- teacher: bfloat16 [65536, 768], P('dp'), may hold values from -6 to 6
- route_to: int32 [65536], P('dp'), may hold values from 0 to 65535, as said below
- anchor: int32 [65536], P('dp'), may hold values from 0 to 65535, as said below
- seq_lengths: int32 [512], P('dp'), may hold values from 0 to 1024, as said below
- query_weight: bfloat16 [768, 768], P('dp'), may hold values from -0.21875 to 0.21875
- query_bias: bfloat16 [768], P('dp'), may hold values from -3 to 3
- key_weight: bfloat16 [768, 768], P('dp'), may hold values from -0.21875 to 0.21875
- value_weight: bfloat16 [768, 768], P('dp'), may hold values from -0.21875 to 0.21875
- value_bias: bfloat16 [768], P('dp'), may hold values from -3 to 3
- out_weight: bfloat16 [768, 768], P('dp'), may hold values from -1.75 to 1.75
- out_bias: bfloat16 [768], P('dp'), may hold values from -3 to 3
- first_gain: bfloat16 [768], P('dp'), may hold values from 0.5 to 1.5
- first_shift: bfloat16 [768], P('dp'), may hold values from -3 to 3
- up_weight: bfloat16 [768, 3072], P('dp'), may hold values from -0.21875 to 0.21875
- up_bias: bfloat16 [3072], P('dp'), may hold values from -3 to 3
- down_weight: bfloat16 [3072, 768], P('dp'), may hold values from -0.109375 to 0.109375
- down_bias: bfloat16 [768], P('dp'), may hold values from -3 to 3
- second_gain: bfloat16 [768], P('dp'), may hold values from 0.5 to 1.5
- second_shift: bfloat16 [768], P('dp'), may hold values from -3 to 3
Outputs:
- states: bfloat16 [65536, 768], P('dp')
- mse_loss: float32 [], replicated
- token_grad: bfloat16 [65536, 768], P('dp')
- grad_query_weight: float32 [768, 768], P('dp')
- grad_query_bias: float32 [768], P('dp')
- grad_key_weight: float32 [768, 768], P('dp')
- grad_value_weight: float32 [768, 768], P('dp')
- grad_value_bias: float32 [768], P('dp')
- grad_out_weight: float32 [768, 768], P('dp')
- grad_out_bias: float32 [768], P('dp')
- grad_first_gain: float32 [768], P('dp')
- grad_first_shift: float32 [768], P('dp')
- grad_up_weight: float32 [768, 3072], P('dp')
- grad_up_bias: float32 [3072], P('dp')
- grad_down_weight: float32 [3072, 768], P('dp')
- grad_down_bias: float32 [768], P('dp')
- grad_second_gain: float32 [768], P('dp')
- grad_second_shift: float32 [768], P('dp')
The draws below stay inside these ranges and needn't reach their ends.
Inputs may be any that keep to these rules, and one draw needn't show every extreme that they name: route_to is a permutation of the rows. Rows k * 2048 to (k + 1) * 2048 - 1 of either order belong to device k; the input rows of each device go to exactly 64 routed rows of every device, and the rows that go from one device to another keep their order. anchor is the inverse of route_to: anchor[route_to[i]] = i. `seq_lengths`: in each aligned group of 8 entries (one micro-batch of one device, in order) the lengths of that micro-batch's sequences come first, zeros follow, and the block counts (L + 127) // 128 of the nonzero lengths L sum to 8; some group holds a single sequence of 1024 rows.
All inputs are finite; a program needn't handle non-finite values.
Results may differ from the reference program's by a relative error of at most 0.013.
Values may be sent and summed in bfloat16 or wider, within the bound.
A program may use at most 256 MiB of HBM per device.

```python
import jax
import jax.numpy as jnp
from jax import lax

D = 768
HEADS = 12
HEAD_DIM = 64
FF = 3072
BLOCK = 128
MICRO = 2
MB_TOK = 1024
TOKENS = 65536
N_DP = 32


def draw_seq_lengths(key, part):
    groups = N_DP * MICRO
    block_count = MB_TOK // BLOCK
    subkeys = jax.random.split(key, 3)
    group_ids = jnp.arange(groups, dtype=jnp.int32)
    device_ids = group_ids // MICRO
    cut_draw = jax.random.randint(subkeys[0], (groups, block_count - 1), 0, N_DP)
    cut_bits = (cut_draw >= device_ids[:, None]).astype(jnp.int32)
    longest = jax.random.randint(subkeys[1], (), 0, groups)
    long_group = group_ids == longest
    cut_bits = jnp.where(long_group[:, None], 0, cut_bits)
    starts = jnp.concatenate([jnp.ones((groups, 1), jnp.int32), cut_bits], axis=1)
    segment = jnp.cumsum(starts, axis=1) - 1
    counts = jnp.sum((segment[:, :, None] == jnp.arange(block_count, dtype=jnp.int32)[None, None, :]).astype(jnp.int32), axis=1)
    shortfall = jax.random.randint(subkeys[2], (groups, block_count), 0, BLOCK)
    tail_rows = BLOCK - shortfall * (N_DP - 1 - device_ids[:, None]) // max(N_DP - 1, 1)
    tail_rows = jnp.where(long_group[:, None], BLOCK, tail_rows)
    lengths = jnp.where(counts > 0, (counts - 1) * BLOCK + tail_rows, 0)
    return lengths.reshape(-1).astype(jnp.int32)


def route_tables(key):
    base = jax.random.fold_in(key, 17)
    rows_dev = MICRO * MB_TOK
    device_count = N_DP
    slot_rows = rows_dev // device_count
    first_key, second_key = jax.random.split(base)
    source_perm = jax.vmap(lambda subkey: jax.random.permutation(subkey, rows_dev))(jax.random.split(first_key, device_count))
    target_perm = jax.vmap(lambda subkey: jax.random.permutation(subkey, rows_dev))(jax.random.split(second_key, device_count))
    source_rows = jnp.sort(source_perm.reshape(device_count, device_count, slot_rows), axis=-1)
    target_rows = jnp.sort(target_perm.reshape(device_count, device_count, slot_rows), axis=-1)
    device_ids = jnp.arange(device_count, dtype=jnp.int32)
    sender = device_ids[:, None, None] * rows_dev + source_rows
    receiver = device_ids[None, :, None] * rows_dev + jnp.transpose(target_rows, (1, 0, 2))
    total_rows = device_count * rows_dev
    routing = jnp.zeros((total_rows,), jnp.int32).at[sender.reshape(-1)].set(receiver.reshape(-1).astype(jnp.int32))
    inverse = jnp.zeros((total_rows,), jnp.int32).at[receiver.reshape(-1)].set(sender.reshape(-1).astype(jnp.int32))
    return (routing, inverse)


def draw_route_to(key, part):
    return route_tables(key)[0]


def draw_anchor(key, part):
    return route_tables(key)[1]


def block_levels(own_key, shape, shards, least, high):
    level = 1.0
    for dim, parts in shards:
        heights = jax.random.uniform(jax.random.fold_in(jax.random.fold_in(own_key, 6), dim), (parts,), jnp.float32, least / len(shards), high / len(shards))
        level = level * jnp.repeat(jnp.exp(heights), shape[dim] // parts).reshape((-1,) + (1,) * (len(shape) - 1 - dim))
    return level


def scatter_about(key, extent, scale, limit, cuts=(), held_as=jnp.bfloat16):
    entries = jax.random.normal(key, extent, jnp.float32) * scale
    if len(cuts) > 0:
        entries = block_levels(key, extent, cuts, -0.22, 0.18) * entries
    return jnp.clip(entries, min=-limit, max=limit).astype(held_as)


def setup_inputs(seed: int = 0) -> dict:
    keys = jax.random.split(jax.random.key(seed), 21)
    return {
        "tokens": scatter_about(keys[0], (TOKENS, D), 1.0, 6.0, ((0, 32),)),
        "teacher": scatter_about(keys[1], (TOKENS, D), 1.0, 6.0, ((0, 32),)),
        "route_to": draw_route_to(jax.random.fold_in(keys[20], 71), 0),
        "anchor": draw_anchor(jax.random.fold_in(keys[20], 71), 0),
        "seq_lengths": draw_seq_lengths(jax.random.fold_in(keys[20], 71), 0),
        "query_weight": scatter_about(keys[5], (D, D), D ** -0.5, 0.21875, ((0, 32),)),
        "query_bias": scatter_about(keys[6], (D,), 0.5, 3.0, ((0, 32),)),
        "key_weight": scatter_about(keys[7], (D, D), D ** -0.5, 0.21875, ((0, 32),)),
        "value_weight": scatter_about(keys[8], (D, D), D ** -0.5, 0.21875, ((0, 32),)),
        "value_bias": scatter_about(keys[9], (D,), 0.5, 3.0, ((0, 32),)),
        "out_weight": scatter_about(keys[10], (D, D), (D // 64) ** -0.5, 1.75, ((0, 32),)),
        "out_bias": scatter_about(keys[11], (D,), 0.5, 3.0, ((0, 32),)),
        "first_gain": jnp.clip(1.0 + 0.1 * jax.random.normal(keys[12], (D,), jnp.float32), 0.5, 1.5).astype(jnp.bfloat16),
        "first_shift": scatter_about(keys[13], (D,), 0.5, 3.0, ((0, 32),)),
        "up_weight": scatter_about(keys[14], (D, FF), D ** -0.5, 0.21875, ((0, 32),)),
        "up_bias": scatter_about(keys[15], (FF,), 0.5, 3.0, ((0, 32),)),
        "down_weight": scatter_about(keys[16], (FF, D), FF ** -0.5, 0.109375, ((0, 32),)),
        "down_bias": scatter_about(keys[17], (D,), 0.5, 3.0, ((0, 32),)),
        "second_gain": jnp.clip(1.0 + 0.1 * jax.random.normal(keys[18], (D,), jnp.float32), 0.5, 1.5).astype(jnp.bfloat16),
        "second_shift": scatter_about(keys[19], (D,), 0.5, 3.0, ((0, 32),)),
    }


@jax.custom_vjp
def low(v):
    return lax.optimization_barrier(v.astype(jnp.bfloat16)).astype(jnp.float32)

@jax.custom_vjp
def low_back(v):
    return v

def low_keep(v):
    return (low(v), None)

def low_pass(kept, grad):
    return (grad,)

def back_keep(v):
    return (v, None)

def back_low(kept, grad):
    return (low(grad),)
low.defvjp(low_keep, low_pass)
low_back.defvjp(back_keep, back_low)
EPSILON = 1e-12

def matmul(left, right):
    return jnp.dot(left, right, precision=lax.Precision.HIGHEST, preferred_element_type=jnp.float32)

def both_ways(value):
    return low_back(low(value))

def layer_norm(value, gain, shift):
    center = value - lax.optimization_barrier(jnp.mean(value, axis=-1, keepdims=True))
    spread = lax.optimization_barrier(jnp.mean(center * center, axis=-1, keepdims=True))
    return center * lax.rsqrt(spread + EPSILON) * gain + shift

def gelu_exact(value):
    return jax.nn.gelu(value, approximate=False)

def sequence_masks(lengths_flat, groups):
    length_grid = lengths_flat.reshape(groups, MB_TOK // BLOCK)
    blocks = (length_grid + BLOCK - 1) // BLOCK
    starts = jnp.cumsum(blocks, axis=1) - blocks
    places = jnp.arange(MB_TOK, dtype=jnp.int32)
    inside = (places[None, :, None] // BLOCK >= starts[:, None, :]) & (blocks[:, None, :] > 0)
    segment = lax.optimization_barrier(jnp.sum(inside.astype(jnp.int32), axis=2)) - 1
    chosen = segment[:, :, None] == jnp.arange(MB_TOK // BLOCK, dtype=jnp.int32)[None, None, :]
    first_row = lax.optimization_barrier(jnp.sum(jnp.where(chosen, starts[:, None, :], 0), axis=2)) * BLOCK
    seq_limit = lax.optimization_barrier(jnp.sum(jnp.where(chosen, length_grid[:, None, :], 0), axis=2))
    usable = places[None, :] - first_row < seq_limit
    return (segment, usable)

def layer_group(params, rows_in, teacher_rows, segment, usable):
    query_weight, query_bias, key_weight, value_weight, value_bias, out_weight, out_bias, first_gain, first_shift, up_weight, up_bias, down_weight, down_bias, second_gain, second_shift = params
    row_count = rows_in.shape[0]
    queries = both_ways((matmul(rows_in, query_weight) + query_bias) * 0.125)
    key_rows = both_ways(matmul(rows_in, key_weight))
    value_rows = both_ways(matmul(rows_in, value_weight) + value_bias)
    head_query = queries.reshape(row_count, HEADS, HEAD_DIM)
    head_key = key_rows.reshape(row_count, HEADS, HEAD_DIM)
    head_value = value_rows.reshape(row_count, HEADS, HEAD_DIM)
    scores = low_back(jnp.einsum('qhd,khd->hqk', head_query, head_key, precision=lax.Precision.HIGHEST))
    allowed = (segment[:, None] == segment[None, :]) & usable[None, :]
    scores = jnp.where(allowed[None], scores, -1e+30)
    attn_probs = jax.nn.softmax(scores, axis=-1)
    attended = jnp.einsum('hqk,khd->qhd', low(attn_probs), head_value, precision=lax.Precision.HIGHEST)
    attended = both_ways(attended.reshape(row_count, HEADS * HEAD_DIM))
    branch = low_back(matmul(attended, out_weight) + out_bias)
    hidden = layer_norm(rows_in + branch, first_gain, first_shift)
    pre_act = low_back(matmul(low(hidden), up_weight) + up_bias)
    activated = low(gelu_exact(pre_act))
    down_out = low_back(matmul(activated, down_weight) + down_bias)
    layer_out = layer_norm(hidden + down_out, second_gain, second_shift)
    misfit = jnp.where(usable[:, None], layer_out - teacher_rows, 0.0)
    return (layer_out, jnp.sum(misfit * misfit))

def reference(tokens, teacher, route_to, anchor, seq_lengths, query_weight, query_bias, key_weight, value_weight, value_bias, out_weight, out_bias, first_gain, first_shift, up_weight, up_bias, down_weight, down_bias, second_gain, second_shift):
    groups = N_DP * MICRO
    params = tuple((param.astype(jnp.float32) for param in (query_weight, query_bias, key_weight, value_weight, value_bias, out_weight, out_bias, first_gain, first_shift, up_weight, up_bias, down_weight, down_bias, second_gain, second_shift)))
    routed_rows = tokens.astype(jnp.float32)[anchor].reshape(groups, MB_TOK, D)
    routed_teacher = teacher.astype(jnp.float32)[anchor].reshape(groups, MB_TOK, D)
    segment, usable = sequence_masks(seq_lengths, groups)
    valid_count = jnp.sum(usable.astype(jnp.float32))

    def objective(param_set, routed):

        def group_step(running, group_data):
            rows_in, teacher_rows, group_segment, group_usable = group_data
            layer_out, squares = jax.checkpoint(layer_group)(param_set, rows_in, teacher_rows, group_segment, group_usable)
            return (running + squares, layer_out)
        squares, outputs = lax.scan(group_step, jnp.zeros((), jnp.float32), (routed, routed_teacher, segment, usable))
        return (squares / valid_count, outputs)
    mse_loss, pullback, outputs = jax.vjp(objective, params, routed_rows, has_aux=True)
    grads, routed_grad = pullback(jnp.asarray(TOKENS, dtype=jnp.float32))
    states = outputs.reshape(TOKENS, D)[route_to].astype(jnp.bfloat16)
    token_grad = routed_grad.reshape(TOKENS, D)[route_to].astype(jnp.bfloat16)
    return (states, mse_loss, token_grad, grads[0], grads[1], grads[2], grads[3], grads[4], grads[5], grads[6], grads[7], grads[8], grads[9], grads[10], grads[11], grads[12], grads[13], grads[14])
```

```python
import functools

import jax
import jax.numpy as jnp
from jax import lax
from jax.experimental import pallas as pl
from jax.experimental.pallas import tpu as pltpu
from jax.sharding import PartitionSpec as P

HEADS = 12
HEAD_DIM = 64
PAIRS = HEADS // 2
LANES = 2 * HEAD_DIM
BLOCK = 128
MB_TOK = 1024
SEQS = MB_TOK // BLOCK
TILE = 256
EPSILON = 1e-12
NEG = -1e30
F32 = jnp.float32
BF16 = jnp.bfloat16


def matmul(left, right):
    return jnp.dot(left, right, preferred_element_type=F32)


def contract_last(left, right):
    return lax.dot_general(left, right, (((1,), (1,)), ((), ())), preferred_element_type=F32)


def cross_rows(left, right):
    return lax.dot_general(left, right, (((0,), (0,)), ((), ())), preferred_element_type=F32)


def column_sum(value):
    return jnp.sum(value, axis=0, dtype=F32)


def sequence_tables(lengths_flat, groups):
    length_grid = lengths_flat.reshape(groups, SEQS)
    blocks = (length_grid + BLOCK - 1) // BLOCK
    before = jnp.arange(SEQS)[:, None] > jnp.arange(SEQS)[None, :]
    starts = jnp.sum(jnp.where(before[None], blocks[:, None, :], 0), axis=2)
    places = jnp.arange(MB_TOK, dtype=jnp.int32)[None, :, None]
    first = (starts * BLOCK)[:, None, :]
    member = (places >= first) & (places < ((starts + blocks) * BLOCK)[:, None, :])
    live = (places >= first) & (places < first + length_grid[:, None, :])
    usable = jnp.any(live, axis=2)
    pad = ((0, 0), (0, 0), (0, HEAD_DIM - SEQS))
    asked = jnp.pad(member.astype(BF16), pad)
    barred = jnp.pad(jnp.where(live, 0.0, NEG).astype(BF16), pad)
    asked = jnp.concatenate([asked, asked], axis=2)
    barred = jnp.concatenate([barred, barred], axis=2)
    rows = groups * MB_TOK
    return asked.reshape(rows, LANES), barred.reshape(rows, LANES), usable.reshape(rows)


def low_half(shape):
    return lax.broadcasted_iota(jnp.int32, shape, 1) < HEAD_DIM


def attend_kernel(q_ref, k_ref, v_ref, asked_ref, barred_ref, out_ref, lse_ref):
    full = low_half((MB_TOK, LANES))
    tile_half = low_half((TILE, LANES))
    ones = jnp.ones((MB_TOK, LANES), BF16)
    keys = k_ref[...]
    barred = barred_ref[...]
    values = v_ref[...]
    keys_of = (jnp.where(full, keys, barred), jnp.where(full, barred, keys))
    values_of = (jnp.where(full, values, ones), jnp.where(full, ones, values))
    for step in range(MB_TOK // TILE):
        rows = pl.ds(step * TILE, TILE)
        queries = q_ref[rows, :]
        asked = asked_ref[rows, :]
        outs = []
        logs = []
        for side in range(2):
            if side == 0:
                query = jnp.where(tile_half, queries, asked)
            else:
                query = jnp.where(tile_half, asked, queries)
            scores = contract_last(query, keys_of[side])
            peak = jnp.max(scores, axis=1, keepdims=True)
            probs = jnp.exp(scores - peak).astype(BF16)
            mixed = matmul(probs, values_of[side])
            total = pltpu.roll(mixed, HEAD_DIM, 1)
            outs.append(mixed / total)
            both = jnp.where(tile_half, total, mixed) if side == 0 else jnp.where(tile_half, mixed, total)
            logs.append(peak + jnp.log(both))
        out_ref[rows, :] = jnp.where(tile_half, outs[0], outs[1]).astype(BF16)
        logs = jnp.where(tile_half, logs[0], logs[1]).T
        lse_ref[0, 0, 0:8, rows] = logs[0:8, :]
        lse_ref[0, 0, 8:16, rows] = logs[HEAD_DIM:HEAD_DIM + 8, :]


def attend(queries, keys, values, asked, barred):
    rows = queries.shape[0]
    micro = rows // MB_TOK
    wide = pl.BlockSpec((MB_TOK, LANES), lambda m, p: (m, p))
    side = pl.BlockSpec((MB_TOK, LANES), lambda m, p: (m, 0))
    return pl.pallas_call(
        attend_kernel,
        grid=(micro, PAIRS),
        in_specs=[wide, wide, wide, side, side],
        out_specs=[wide, pl.BlockSpec((1, 1, 16, MB_TOK), lambda m, p: (m, p, 0, 0))],
        out_shape=(
            jax.ShapeDtypeStruct(queries.shape, BF16),
            jax.ShapeDtypeStruct((micro, PAIRS, 16, MB_TOK), F32),
        ),
        compiler_params=pltpu.CompilerParams(vmem_limit_bytes=56 << 20),
        cost_estimate=pl.CostEstimate(
            flops=4 * rows * MB_TOK * HEADS * HEAD_DIM,
            transcendentals=rows * MB_TOK * HEADS,
            bytes_accessed=rows * 768 * 8,
        ),
        name="attend",
    )(queries, keys, values, asked, barred)


def attend_back_kernel(q_ref, k_ref, v_ref, g_ref, lse_ref, asked_ref, barred_ref, dq_ref, dk_ref, dv_ref, acc_k, acc_v):
    full = low_half((MB_TOK, LANES))
    tile_half = low_half((TILE, LANES))
    keys = k_ref[...]
    barred = barred_ref[...]
    values = v_ref[...]
    zero = jnp.zeros_like(values)
    keys_of = (jnp.where(full, keys, barred), jnp.where(full, barred, keys))
    values_of = (jnp.where(full, values, zero), jnp.where(full, zero, values))
    keys_turned = keys.astype(F32).T.astype(BF16)
    for step in range(MB_TOK // TILE):
        rows = pl.ds(step * TILE, TILE)
        queries = q_ref[rows, :]
        asked = asked_ref[rows, :]
        grads = g_ref[rows, :]
        turned = []
        for side in range(2):
            if side == 0:
                query = jnp.where(tile_half, queries, asked)
            else:
                query = jnp.where(tile_half, asked, queries)
            scores = contract_last(keys_of[side], query)
            probs = jnp.exp(scores - lse_ref[0, 0, 8 * side:8 * side + 1, rows])
            grad_probs = contract_last(values_of[side], grads)
            product = probs * grad_probs
            centre = jnp.sum(product, axis=0, keepdims=True)
            grad_scores = (product - probs * centre).astype(BF16)
            part_v = matmul(probs.astype(BF16), grads)
            part_k = matmul(grad_scores, queries)
            if step == 0:
                acc_v[side] = part_v
                acc_k[side] = part_k
            else:
                acc_v[side] += part_v
                acc_k[side] += part_k
            turned.append(matmul(keys_turned[side * HEAD_DIM:(side + 1) * HEAD_DIM, :], grad_scores))
        dq_ref[rows, :] = jnp.concatenate(turned, axis=0).T.astype(BF16)
    dk_ref[...] = jnp.where(full, acc_k[0], acc_k[1]).astype(BF16)
    dv_ref[...] = jnp.where(full, acc_v[0], acc_v[1]).astype(BF16)


def attend_back(queries, keys, values, grads, lse, asked, barred):
    rows = queries.shape[0]
    micro = rows // MB_TOK
    wide = pl.BlockSpec((MB_TOK, LANES), lambda m, p: (m, p))
    side = pl.BlockSpec((MB_TOK, LANES), lambda m, p: (m, 0))
    return pl.pallas_call(
        attend_back_kernel,
        grid=(micro, PAIRS),
        in_specs=[wide, wide, wide, wide, pl.BlockSpec((1, 1, 16, MB_TOK), lambda m, p: (m, p, 0, 0)), side, side],
        out_specs=[wide, wide, wide],
        out_shape=(jax.ShapeDtypeStruct(queries.shape, BF16),) * 3,
        scratch_shapes=[pltpu.VMEM((2, MB_TOK, LANES), F32), pltpu.VMEM((2, MB_TOK, LANES), F32)],
        compiler_params=pltpu.CompilerParams(vmem_limit_bytes=56 << 20),
        cost_estimate=pl.CostEstimate(
            flops=10 * rows * MB_TOK * HEADS * HEAD_DIM,
            transcendentals=rows * MB_TOK * HEADS,
            bytes_accessed=rows * 768 * 14,
        ),
        name="attend_back",
    )(queries, keys, values, grads, lse, asked, barred)


def norm_stats(value):
    center = value - jnp.mean(value, axis=-1, keepdims=True)
    spread = jnp.mean(center * center, axis=-1, keepdims=True)
    scale = lax.rsqrt(spread + EPSILON)
    return center * scale, scale


def norm_back(grad, normed, scale, gain):
    u = grad * gain
    return scale * (
        u
        - jnp.mean(u, axis=-1, keepdims=True)
        - normed * jnp.mean(u * normed, axis=-1, keepdims=True)
    )


def slot_positions(targets, rows_dev, slot_rows, device_count):
    owner_dev = targets // rows_dev
    onehot = (owner_dev[:, None] == jnp.arange(device_count, dtype=jnp.int32)[None, :]).astype(
        jnp.int32
    )
    ranking = jnp.sum(jnp.cumsum(onehot, axis=0) * onehot, axis=1) - 1
    return owner_dev * slot_rows + ranking


def invert(positions):
    return (
        jnp.zeros_like(positions).at[positions].set(jnp.arange(positions.shape[0], dtype=jnp.int32))
    )


def exchange(rows, device_count):
    count, width = rows.shape
    return lax.all_to_all(
        rows.reshape(device_count, count // device_count, width), "dp", split_axis=0, concat_axis=0, tiled=True
    ).reshape(count, width)


def on_device(
    tokens,
    teacher,
    route_to,
    anchor,
    seq_lengths,
    query_weight,
    query_bias,
    key_weight,
    value_weight,
    value_bias,
    out_weight,
    out_bias,
    first_gain,
    first_shift,
    up_weight,
    up_bias,
    down_weight,
    down_bias,
    second_gain,
    second_shift,
):
    rows_dev, width = tokens.shape
    device_count = lax.axis_size("dp")
    slot_rows = rows_dev // device_count
    micro_count = rows_dev // MB_TOK
    asked, barred, usable = sequence_tables(seq_lengths, micro_count)

    count = jnp.sum(seq_lengths)
    pieces = jnp.stack([count // 64, count % 64]).astype(BF16)
    vectors = (query_bias, value_bias, out_bias, first_gain, first_shift, down_bias, second_gain, second_shift, up_bias)
    sizes = [v.shape[0] for v in vectors]
    used = sum(sizes) + 2
    padded = -(-used // 128) * 128
    packed = jnp.concatenate(list(vectors) + [pieces, jnp.zeros((padded - used,), BF16)])
    gathered = lax.all_gather(packed, "dp", axis=0, tiled=False).astype(F32)
    full_vectors = []
    place = 0
    for size in sizes:
        full_vectors.append(gathered[:, place:place + size].reshape(-1))
        place += size
    q_b, v_b, o_b, g1, s1, d_b, g2, s2, u_b = full_vectors
    valid_count = jnp.sum(gathered[:, place] * 64.0 + gathered[:, place + 1])

    w_qkv = lax.all_gather(
        jnp.concatenate([query_weight, key_weight, value_weight], axis=1), "dp", axis=0, tiled=True
    )
    w_out = lax.all_gather(out_weight, "dp", axis=0, tiled=True)
    w_up = lax.all_gather(up_weight, "dp", axis=0, tiled=True)
    w_down = lax.all_gather(down_weight, "dp", axis=0, tiled=True)

    outgoing = slot_positions(route_to, rows_dev, slot_rows, device_count)
    incoming = slot_positions(anchor, rows_dev, slot_rows, device_count)
    send_order = invert(outgoing)
    back_order = invert(incoming)
    x = exchange(tokens[send_order], device_count)[incoming]
    target = exchange(teacher[send_order], device_count)[incoming]

    w_q = w_qkv[:, :width]
    w_k = w_qkv[:, width:2 * width]
    w_v = w_qkv[:, 2 * width:]
    queries = ((matmul(x, w_q) + q_b) * 0.125).astype(BF16)
    keys = matmul(x, w_k).astype(BF16)
    values = (matmul(x, w_v) + v_b).astype(BF16)
    attended, lse = attend(queries, keys, values, asked, barred)
    pre_first = x + (matmul(attended, w_out) + o_b)
    n1, r1 = norm_stats(pre_first)
    hidden = n1 * g1 + s1
    hidden_low = hidden.astype(BF16)
    pre_act = matmul(hidden_low, w_up) + u_b
    cdf = 0.5 * (1.0 + lax.erf(pre_act * (2.0 ** -0.5)))
    act_low = (pre_act * cdf).astype(BF16)
    slope = (cdf + pre_act * (jnp.exp(-0.5 * pre_act * pre_act) * 0.3989422804014327)).astype(BF16)
    pre_second = hidden + (matmul(act_low, w_down) + d_b)
    n2, r2 = norm_stats(pre_second)
    layer_out = n2 * g2 + s2
    misfit = jnp.where(usable[:, None], layer_out - target.astype(F32), 0.0)
    states_routed = layer_out.astype(BF16)
    squares = jnp.sum(misfit * misfit)
    states = exchange(states_routed[back_order], device_count)[outgoing]

    grad_out = misfit * (rows_dev * device_count * 2.0 / valid_count)
    grad_s2 = column_sum(grad_out)
    grad_g2 = column_sum(grad_out * n2)
    grad_pre_second = norm_back(grad_out, n2, r2, g2)
    down_grad = grad_pre_second.astype(BF16)
    grad_w_down = cross_rows(act_low, down_grad).astype(BF16)
    grad_d_b = column_sum(down_grad)
    up_grad = (slope * contract_last(down_grad, w_down)).astype(BF16)
    grad_w_up = cross_rows(hidden_low, up_grad).astype(BF16)
    grad_u_b = column_sum(up_grad)
    share_down = lax.psum_scatter(grad_w_down, "dp", scatter_dimension=0, tiled=True)
    share_up = lax.psum_scatter(grad_w_up, "dp", scatter_dimension=0, tiled=True)
    grad_hidden = grad_pre_second + contract_last(up_grad, w_up)
    grad_s1 = column_sum(grad_hidden)
    grad_g1 = column_sum(grad_hidden * n1)
    grad_pre_first = norm_back(grad_hidden, n1, r1, g1)
    out_grad = grad_pre_first.astype(BF16)
    grad_w_out = cross_rows(attended, out_grad).astype(BF16)
    grad_o_b = column_sum(out_grad)
    share_out = lax.psum_scatter(grad_w_out, "dp", scatter_dimension=0, tiled=True)
    attended_grad = contract_last(out_grad, w_out).astype(BF16)
    dq, dk, dv = attend_back(queries, keys, values, attended_grad, lse, asked, barred)
    dq = dq * jnp.asarray(0.125, BF16)
    rows_grad = (
        grad_pre_first + contract_last(dq, w_q) + contract_last(dk, w_k) + contract_last(dv, w_v)
    ).astype(BF16)
    token_grad = exchange(rows_grad[back_order], device_count)[outgoing]
    grad_q_b = column_sum(dq)
    grad_v_b = column_sum(dv)
    grad_w_qkv = jnp.concatenate(
        [cross_rows(x, dq).astype(BF16), cross_rows(x, dk).astype(BF16), cross_rows(x, dv).astype(BF16)], axis=1
    )
    share_qkv = lax.psum_scatter(grad_w_qkv, "dp", scatter_dimension=0, tiled=True).astype(F32)

    grad_vectors = (grad_q_b, grad_v_b, grad_o_b, grad_g1, grad_s1, grad_d_b, grad_g2, grad_s2, grad_u_b)
    total_block = jnp.broadcast_to(squares.reshape(1, 1), (device_count, 1))
    grad_used = sum(sizes) + 1
    fill = jnp.zeros((device_count, -(-grad_used // 128) * 128 - grad_used), F32)
    grad_packed = jnp.concatenate(
        [g.reshape(device_count, -1) for g in grad_vectors] + [total_block, fill], axis=1
    )
    summed = lax.psum_scatter(grad_packed, "dp", scatter_dimension=0, tiled=True).reshape(-1)
    parts = []
    place = 0
    for size in sizes:
        parts.append(summed[place:place + size])
        place += size
    h_q_b, h_v_b, h_o_b, h_g1, h_s1, h_d_b, h_g2, h_s2, h_u_b = parts
    mse_loss = summed[place] / valid_count
    return (
        states,
        mse_loss,
        token_grad,
        share_qkv[:, :width],
        h_q_b,
        share_qkv[:, width:2 * width],
        share_qkv[:, 2 * width:],
        h_v_b,
        share_out.astype(F32),
        h_o_b,
        h_g1,
        h_s1,
        share_up.astype(F32),
        h_u_b,
        share_down.astype(F32),
        h_d_b,
        h_g2,
        h_s2,
    )


def solution(mesh):
    row = P("dp", None)
    vec = P("dp")
    placed = (row, row, vec, vec, vec, row, vec, row, row, vec, row, vec, vec, vec, row, vec, row, vec, vec, vec)
    return jax.shard_map(
        on_device,
        mesh=mesh,
        in_specs=placed,
        out_specs=(row, P(), row, row, vec, row, row, vec, row, vec, vec, vec, row, vec, row, vec, vec, vec),
        check_vma=False,
    )
```

```python
import jax
import jax.numpy as jnp
from jax import lax
from jax.experimental import pallas as pl
from jax.experimental.pallas import tpu as pltpu
from jax.sharding import PartitionSpec as P


HEADS = 12
HEAD_DIM = 64
PAIRS = HEADS // 2
LANES = 2 * HEAD_DIM
BLOCK = 128
MB_TOK = 1024
SEQS = MB_TOK // BLOCK
TILE = 256
EPSILON = 1e-12
NEG = -1e30
F32 = jnp.float32
BF16 = jnp.bfloat16


def matmul(left, right):
    return jnp.dot(left, right, preferred_element_type=F32)


def contract_last(left, right):
    return lax.dot_general(left, right, (((1,), (1,)), ((), ())), preferred_element_type=F32)


def cross_rows(left, right):
    return lax.dot_general(left, right, (((0,), (0,)), ((), ())), preferred_element_type=F32)


def column_sum(value):
    return jnp.sum(value, axis=0, dtype=F32)


def sequence_tables(lengths_flat, groups):
    length_grid = lengths_flat.reshape(groups, SEQS)
    blocks = (length_grid + BLOCK - 1) // BLOCK
    before = jnp.arange(SEQS)[:, None] > jnp.arange(SEQS)[None, :]
    starts = jnp.sum(jnp.where(before[None], blocks[:, None, :], 0), axis=2)
    places = jnp.arange(MB_TOK, dtype=jnp.int32)[None, :, None]
    first = (starts * BLOCK)[:, None, :]
    member = (places >= first) & (places < ((starts + blocks) * BLOCK)[:, None, :])
    live = (places >= first) & (places < first + length_grid[:, None, :])
    usable = jnp.any(live, axis=2)
    pad = ((0, 0), (0, 0), (0, HEAD_DIM - SEQS))
    asked = jnp.pad(member.astype(BF16), pad)
    barred = jnp.pad(jnp.where(live, 0.0, NEG).astype(BF16), pad)
    asked = jnp.concatenate([asked, asked], axis=2)
    barred = jnp.concatenate([barred, barred], axis=2)
    rows = groups * MB_TOK
    return asked.reshape(rows, LANES), barred.reshape(rows, LANES), usable.reshape(rows)


def low_half(shape):
    return lax.broadcasted_iota(jnp.int32, shape, 1) < HEAD_DIM


def attend_kernel(q_ref, k_ref, v_ref, asked_ref, barred_ref, out_ref, lse_ref):
    full = low_half((MB_TOK, LANES))
    tile_half = low_half((TILE, LANES))
    ones = jnp.ones((MB_TOK, LANES), BF16)
    keys = k_ref[...]
    barred = barred_ref[...]
    values = v_ref[...]
    keys_of = (jnp.where(full, keys, barred), jnp.where(full, barred, keys))
    values_of = (jnp.where(full, values, ones), jnp.where(full, ones, values))
    for step in range(MB_TOK // TILE):
        rows = pl.ds(step * TILE, TILE)
        queries = q_ref[rows, :]
        asked = asked_ref[rows, :]
        outs = []
        logs = []
        for side in range(2):
            if side == 0:
                query = jnp.where(tile_half, queries, asked)
            else:
                query = jnp.where(tile_half, asked, queries)
            scores = contract_last(query, keys_of[side])
            peak = jnp.max(scores, axis=1, keepdims=True)
            probs = jnp.exp(scores - peak).astype(BF16)
            mixed = matmul(probs, values_of[side])
            total = pltpu.roll(mixed, HEAD_DIM, 1)
            outs.append(mixed / total)
            both = jnp.where(tile_half, total, mixed) if side == 0 else jnp.where(tile_half, mixed, total)
            logs.append(peak + jnp.log(both))
        out_ref[rows, :] = jnp.where(tile_half, outs[0], outs[1]).astype(BF16)
        logs = jnp.where(tile_half, logs[0], logs[1]).T
        lse_ref[0, 0, 0:8, rows] = logs[0:8, :]
        lse_ref[0, 0, 8:16, rows] = logs[HEAD_DIM:HEAD_DIM + 8, :]


def attend(queries, keys, values, asked, barred):
    rows = queries.shape[0]
    micro = rows // MB_TOK
    wide = pl.BlockSpec((MB_TOK, LANES), lambda m, p: (m, p))
    side = pl.BlockSpec((MB_TOK, LANES), lambda m, p: (m, 0))
    return pl.pallas_call(
        attend_kernel,
        grid=(micro, PAIRS),
        in_specs=[wide, wide, wide, side, side],
        out_specs=[wide, pl.BlockSpec((1, 1, 16, MB_TOK), lambda m, p: (m, p, 0, 0))],
        out_shape=(
            jax.ShapeDtypeStruct(queries.shape, BF16),
            jax.ShapeDtypeStruct((micro, PAIRS, 16, MB_TOK), F32),
        ),
        compiler_params=pltpu.CompilerParams(vmem_limit_bytes=56 << 20),
        cost_estimate=pl.CostEstimate(
            flops=4 * rows * MB_TOK * HEADS * HEAD_DIM,
            transcendentals=rows * MB_TOK * HEADS,
            bytes_accessed=rows * 768 * 8,
        ),
        name="attend",
    )(queries, keys, values, asked, barred)


def attend_back_kernel(q_ref, k_ref, v_ref, g_ref, lse_ref, asked_ref, barred_ref, dq_ref, dk_ref, dv_ref, acc_k, acc_v):
    full = low_half((MB_TOK, LANES))
    tile_half = low_half((TILE, LANES))
    keys = k_ref[...]
    barred = barred_ref[...]
    values = v_ref[...]
    zero = jnp.zeros_like(values)
    keys_of = (jnp.where(full, keys, barred), jnp.where(full, barred, keys))
    values_of = (jnp.where(full, values, zero), jnp.where(full, zero, values))
    keys_turned = keys.astype(F32).T.astype(BF16)
    for step in range(MB_TOK // TILE):
        rows = pl.ds(step * TILE, TILE)
        queries = q_ref[rows, :]
        asked = asked_ref[rows, :]
        grads = g_ref[rows, :]
        turned = []
        for side in range(2):
            if side == 0:
                query = jnp.where(tile_half, queries, asked)
            else:
                query = jnp.where(tile_half, asked, queries)
            scores = contract_last(keys_of[side], query)
            probs = jnp.exp(scores - lse_ref[0, 0, 8 * side:8 * side + 1, rows])
            grad_probs = contract_last(values_of[side], grads)
            product = probs * grad_probs
            centre = jnp.sum(product, axis=0, keepdims=True)
            grad_scores = (product - probs * centre).astype(BF16)
            part_v = matmul(probs.astype(BF16), grads)
            part_k = matmul(grad_scores, queries)
            if step == 0:
                acc_v[side] = part_v
                acc_k[side] = part_k
            else:
                acc_v[side] += part_v
                acc_k[side] += part_k
            turned.append(matmul(keys_turned[side * HEAD_DIM:(side + 1) * HEAD_DIM, :], grad_scores))
        dq_ref[rows, :] = jnp.concatenate(turned, axis=0).T.astype(BF16)
    dk_ref[...] = jnp.where(full, acc_k[0], acc_k[1]).astype(BF16)
    dv_ref[...] = jnp.where(full, acc_v[0], acc_v[1]).astype(BF16)


def attend_back(queries, keys, values, grads, lse, asked, barred):
    rows = queries.shape[0]
    micro = rows // MB_TOK
    wide = pl.BlockSpec((MB_TOK, LANES), lambda m, p: (m, p))
    side = pl.BlockSpec((MB_TOK, LANES), lambda m, p: (m, 0))
    return pl.pallas_call(
        attend_back_kernel,
        grid=(micro, PAIRS),
        in_specs=[wide, wide, wide, wide, pl.BlockSpec((1, 1, 16, MB_TOK), lambda m, p: (m, p, 0, 0)), side, side],
        out_specs=[wide, wide, wide],
        out_shape=(jax.ShapeDtypeStruct(queries.shape, BF16),) * 3,
        scratch_shapes=[pltpu.VMEM((2, MB_TOK, LANES), F32), pltpu.VMEM((2, MB_TOK, LANES), F32)],
        compiler_params=pltpu.CompilerParams(vmem_limit_bytes=56 << 20),
        cost_estimate=pl.CostEstimate(
            flops=10 * rows * MB_TOK * HEADS * HEAD_DIM,
            transcendentals=rows * MB_TOK * HEADS,
            bytes_accessed=rows * 768 * 14,
        ),
        name="attend_back",
    )(queries, keys, values, grads, lse, asked, barred)


def norm_stats(value):
    center = value - jnp.mean(value, axis=-1, keepdims=True)
    spread = jnp.mean(center * center, axis=-1, keepdims=True)
    scale = lax.rsqrt(spread + EPSILON)
    return center * scale, scale


def norm_back(grad, normed, scale, gain):
    u = grad * gain
    return scale * (
        u
        - jnp.mean(u, axis=-1, keepdims=True)
        - normed * jnp.mean(u * normed, axis=-1, keepdims=True)
    )


def slot_positions(targets, rows_dev, slot_rows, device_count):
    owner_dev = targets // rows_dev
    chunks = rows_dev // BLOCK
    onehot = (owner_dev[:, None] == jnp.arange(device_count, dtype=jnp.int32)[None, :]).astype(BF16)
    onehot = onehot.reshape(chunks, BLOCK, device_count)
    steps = jnp.arange(BLOCK)
    earlier = (steps[:, None] > steps[None, :]).astype(BF16)
    inner = jnp.einsum("ij,cjd->cid", earlier, onehot, preferred_element_type=F32)
    sums = jnp.sum(onehot.astype(F32), axis=1)
    places = jnp.arange(chunks)
    outer = jnp.sum(jnp.where((places[:, None] > places[None, :])[:, :, None], sums[None], 0.0), axis=1)
    rank = jnp.sum((inner + outer[:, None, :]) * onehot.astype(F32), axis=2)
    return owner_dev * slot_rows + rank.reshape(rows_dev).astype(jnp.int32)


def invert(positions):
    return (
        jnp.zeros_like(positions).at[positions].set(jnp.arange(positions.shape[0], dtype=jnp.int32))
    )


def gather(value, tiled=True):
    return lax.all_gather(value, "dp", axis=0, tiled=tiled)


def scatter_sum(value):
    return lax.psum_scatter(value, "dp", scatter_dimension=0, tiled=True)


def exchange(rows, device_count):
    count, width = rows.shape
    slots = rows.reshape(device_count, count // device_count, width)
    slots = lax.all_to_all(slots, "dp", split_axis=0, concat_axis=0, tiled=True)
    return slots.reshape(count, width)


def layer_step(
    tokens,
    teacher,
    route_to,
    anchor,
    seq_lengths,
    query_weight,
    query_bias,
    key_weight,
    value_weight,
    value_bias,
    out_weight,
    out_bias,
    first_gain,
    first_shift,
    up_weight,
    up_bias,
    down_weight,
    down_bias,
    second_gain,
    second_shift,
):
    rows_dev, width = tokens.shape
    device_count = lax.axis_size("dp")
    slot_rows = rows_dev // device_count
    micro_count = rows_dev // MB_TOK
    asked, barred, usable = sequence_tables(seq_lengths, micro_count)

    count = jnp.sum(seq_lengths)
    pieces = jnp.stack([count // 64, count % 64]).astype(BF16)
    vectors = (query_bias, value_bias, out_bias, first_gain, first_shift, down_bias, second_gain, second_shift, up_bias)
    sizes = [v.shape[0] for v in vectors]
    used = sum(sizes) + 2
    extra = -(-used // width)
    packed = jnp.concatenate(list(vectors) + [pieces, jnp.zeros((extra * width - used,), BF16)])
    own_out = out_weight.shape[0]
    w_qkv = gather(jnp.concatenate([query_weight, key_weight, value_weight], axis=1))
    with_out = gather(jnp.concatenate([out_weight, packed.reshape(extra, width)], axis=0), False)
    w_out = with_out[:, :own_out].reshape(device_count * own_out, width)
    gathered = with_out[:, own_out:].reshape(device_count, extra * width).astype(F32)
    w_up = gather(up_weight)
    w_down = gather(down_weight)
    full_vectors = []
    place = 0
    for size in sizes:
        full_vectors.append(gathered[:, place:place + size].reshape(-1))
        place += size
    q_b, v_b, o_b, g1, s1, d_b, g2, s2, u_b = full_vectors
    valid_count = jnp.sum(gathered[:, place] * 64.0 + gathered[:, place + 1])

    outgoing = slot_positions(route_to, rows_dev, slot_rows, device_count)
    incoming = slot_positions(anchor, rows_dev, slot_rows, device_count)
    send_order = invert(outgoing)
    back_order = invert(incoming)
    tokens_out, incoming, back_order = lax.optimization_barrier((tokens[send_order], incoming, back_order))
    x = exchange(tokens_out, device_count)[incoming]
    target = exchange(teacher[send_order], device_count)[incoming]

    w_q = w_qkv[:, :width]
    w_k = w_qkv[:, width:2 * width]
    w_v = w_qkv[:, 2 * width:]
    queries = ((matmul(x, w_q) + q_b) * 0.125).astype(BF16)
    keys = matmul(x, w_k).astype(BF16)
    values = (matmul(x, w_v) + v_b).astype(BF16)
    attended, lse = attend(queries, keys, values, asked, barred)
    pre_first = x + (matmul(attended, w_out) + o_b)
    n1, r1 = norm_stats(pre_first)
    hidden = n1 * g1 + s1
    hidden_low = hidden.astype(BF16)
    pre_act = matmul(hidden_low, w_up) + u_b
    cdf = 0.5 * (1.0 + lax.erf(pre_act * (2.0 ** -0.5)))
    act_low = (pre_act * cdf).astype(BF16)
    slope = (cdf + pre_act * (jnp.exp(-0.5 * pre_act * pre_act) * 0.3989422804014327)).astype(BF16)
    pre_second = hidden + (matmul(act_low, w_down) + d_b)
    n2, r2 = norm_stats(pre_second)
    layer_out = n2 * g2 + s2
    misfit = jnp.where(usable[:, None], layer_out - target.astype(F32), 0.0)
    states_routed = layer_out.astype(BF16)
    squares = jnp.sum(misfit * misfit)
    states_out = states_routed[back_order]

    grad_out = misfit * (rows_dev * device_count * 2.0 / valid_count)
    grad_s2 = column_sum(grad_out)
    grad_g2 = column_sum(grad_out * n2)
    grad_pre_second = norm_back(grad_out, n2, r2, g2)
    down_grad, states_out = lax.optimization_barrier((grad_pre_second.astype(BF16), states_out))
    states = exchange(states_out, device_count)[outgoing]
    grad_w_down = cross_rows(act_low, down_grad).astype(BF16)
    grad_d_b = column_sum(down_grad)
    up_grad = (slope * contract_last(down_grad, w_down)).astype(BF16)
    grad_w_up = cross_rows(hidden_low, up_grad).astype(BF16)
    grad_u_b = column_sum(up_grad)
    grad_hidden = grad_pre_second + contract_last(up_grad, w_up)
    grad_s1 = column_sum(grad_hidden)
    grad_g1 = column_sum(grad_hidden * n1)
    grad_pre_first = norm_back(grad_hidden, n1, r1, g1)
    out_grad = grad_pre_first.astype(BF16)
    grad_w_out = cross_rows(attended, out_grad).astype(BF16)
    grad_o_b = column_sum(out_grad)
    attended_grad = contract_last(out_grad, w_out).astype(BF16)
    attended_grad, grad_w_down, grad_w_up, grad_w_out = lax.optimization_barrier(
        (attended_grad, grad_w_down, grad_w_up, grad_w_out)
    )
    share_down = scatter_sum(grad_w_down)
    share_up = scatter_sum(grad_w_up)
    share_out = scatter_sum(grad_w_out)
    dq, dk, dv = attend_back(queries, keys, values, attended_grad, lse, asked, barred)
    dq = dq * jnp.asarray(0.125, BF16)
    rows_grad = (
        grad_pre_first + contract_last(dq, w_q) + contract_last(dk, w_k) + contract_last(dv, w_v)
    ).astype(BF16)
    token_grad = exchange(rows_grad[back_order], device_count)[outgoing]
    grad_q_b = column_sum(dq)
    grad_v_b = column_sum(dv)
    grad_w_qkv = jnp.concatenate(
        [cross_rows(x, dq).astype(BF16), cross_rows(x, dk).astype(BF16), cross_rows(x, dv).astype(BF16)], axis=1
    )
    share_qkv = scatter_sum(grad_w_qkv).astype(F32)

    grad_vectors = (grad_q_b, grad_v_b, grad_o_b, grad_g1, grad_s1, grad_d_b, grad_g2, grad_s2, grad_u_b)
    total_block = jnp.broadcast_to(squares.reshape(1, 1), (device_count, 1))
    grad_used = sum(sizes) + 1
    fill = jnp.zeros((device_count, -(-grad_used // 128) * 128 - grad_used), F32)
    grad_packed = jnp.concatenate(
        [g.reshape(device_count, -1) for g in grad_vectors] + [total_block, fill], axis=1
    )
    shares = lax.all_to_all(grad_packed, "dp", split_axis=0, concat_axis=0, tiled=True)
    summed = jnp.sum(shares, axis=0)
    parts = []
    place = 0
    for size in sizes:
        parts.append(summed[place:place + size])
        place += size
    h_q_b, h_v_b, h_o_b, h_g1, h_s1, h_d_b, h_g2, h_s2, h_u_b = parts
    mse_loss = summed[place] / valid_count
    return (
        states,
        mse_loss,
        token_grad,
        share_qkv[:, :width],
        h_q_b,
        share_qkv[:, width:2 * width],
        share_qkv[:, 2 * width:],
        h_v_b,
        share_out.astype(F32),
        h_o_b,
        h_g1,
        h_s1,
        share_up.astype(F32),
        h_u_b,
        share_down.astype(F32),
        h_d_b,
        h_g2,
        h_s2,
    )


def solution(mesh):
    row = P("dp", None)
    vec = P("dp")
    placed = (row, row, vec, vec, vec, row, vec, row, row, vec, row, vec, vec, vec, row, vec, row, vec, vec, vec)
    return jax.shard_map(
        layer_step,
        mesh=mesh,
        in_specs=placed,
        out_specs=(row, P(), row, row, vec, row, row, vec, row, vec, vec, vec, row, vec, row, vec, vec, vec),
        check_vma=False,
    )
```

```python
import jax
import jax.numpy as jnp
from jax import lax
from jax.experimental import pallas as pl
from jax.experimental.pallas import tpu as pltpu
from jax.sharding import PartitionSpec as P


HEADS = 12
HEAD_DIM = 64
PAIRS = HEADS // 2
LANES = 2 * HEAD_DIM
BLOCK = 128
MB_TOK = 1024
SEQS = MB_TOK // BLOCK
TILE = 256
EPSILON = 1e-12
NEG = -1e30
F32 = jnp.float32
BF16 = jnp.bfloat16


def matmul(left, right):
    return jnp.dot(left, right, preferred_element_type=F32)


def contract_last(left, right):
    return lax.dot_general(left, right, (((1,), (1,)), ((), ())), preferred_element_type=F32)


def cross_rows(left, right):
    return lax.dot_general(left, right, (((0,), (0,)), ((), ())), preferred_element_type=F32)


def column_sum(value):
    return jnp.sum(value, axis=0, dtype=F32)


def sequence_tables(lengths_flat, groups):
    length_grid = lengths_flat.reshape(groups, SEQS)
    blocks = (length_grid + BLOCK - 1) // BLOCK
    before = jnp.arange(SEQS)[:, None] > jnp.arange(SEQS)[None, :]
    starts = jnp.sum(jnp.where(before[None], blocks[:, None, :], 0), axis=2)
    places = jnp.arange(MB_TOK, dtype=jnp.int32)[None, :, None]
    first = (starts * BLOCK)[:, None, :]
    member = (places >= first) & (places < ((starts + blocks) * BLOCK)[:, None, :])
    live = (places >= first) & (places < first + length_grid[:, None, :])
    usable = jnp.any(live, axis=2)
    pad = ((0, 0), (0, 0), (0, HEAD_DIM - SEQS))
    asked = jnp.pad(member.astype(BF16), pad)
    barred = jnp.pad(jnp.where(live, 0.0, NEG).astype(BF16), pad)
    asked = jnp.concatenate([asked, asked], axis=2)
    barred = jnp.concatenate([barred, barred], axis=2)
    rows = groups * MB_TOK
    return asked.reshape(rows, LANES), barred.reshape(rows, LANES), usable.reshape(rows)


def low_half(shape):
    return lax.broadcasted_iota(jnp.int32, shape, 1) < HEAD_DIM


def attend_kernel(q_ref, k_ref, v_ref, asked_ref, barred_ref, out_ref, lse_ref):
    full = low_half((MB_TOK, LANES))
    tile_half = low_half((TILE, LANES))
    ones = jnp.ones((MB_TOK, LANES), BF16)
    keys = k_ref[...]
    barred = barred_ref[...]
    values = v_ref[...]
    keys_of = (jnp.where(full, keys, barred), jnp.where(full, barred, keys))
    values_of = (jnp.where(full, values, ones), jnp.where(full, ones, values))
    for step in range(MB_TOK // TILE):
        rows = pl.ds(step * TILE, TILE)
        queries = q_ref[rows, :]
        asked = asked_ref[rows, :]
        outs = []
        logs = []
        for side in range(2):
            if side == 0:
                query = jnp.where(tile_half, queries, asked)
            else:
                query = jnp.where(tile_half, asked, queries)
            scores = contract_last(query, keys_of[side])
            peak = jnp.max(scores, axis=1, keepdims=True)
            probs = jnp.exp(scores - peak).astype(BF16)
            mixed = matmul(probs, values_of[side])
            total = pltpu.roll(mixed, HEAD_DIM, 1)
            outs.append(mixed / total)
            both = jnp.where(tile_half, total, mixed) if side == 0 else jnp.where(tile_half, mixed, total)
            logs.append(peak + jnp.log(both))
        out_ref[rows, :] = jnp.where(tile_half, outs[0], outs[1]).astype(BF16)
        logs = jnp.where(tile_half, logs[0], logs[1]).T
        lse_ref[0, 0, 0:8, rows] = logs[0:8, :]
        lse_ref[0, 0, 8:16, rows] = logs[HEAD_DIM:HEAD_DIM + 8, :]


def attend(queries, keys, values, asked, barred):
    rows = queries.shape[0]
    micro = rows // MB_TOK
    wide = pl.BlockSpec((MB_TOK, LANES), lambda m, p: (m, p))
    side = pl.BlockSpec((MB_TOK, LANES), lambda m, p: (m, 0))
    return pl.pallas_call(
        attend_kernel,
        grid=(micro, PAIRS),
        in_specs=[wide, wide, wide, side, side],
        out_specs=[wide, pl.BlockSpec((1, 1, 16, MB_TOK), lambda m, p: (m, p, 0, 0))],
        out_shape=(
            jax.ShapeDtypeStruct(queries.shape, BF16),
            jax.ShapeDtypeStruct((micro, PAIRS, 16, MB_TOK), F32),
        ),
        compiler_params=pltpu.CompilerParams(vmem_limit_bytes=56 << 20),
        cost_estimate=pl.CostEstimate(
            flops=4 * rows * MB_TOK * HEADS * HEAD_DIM,
            transcendentals=rows * MB_TOK * HEADS,
            bytes_accessed=rows * 768 * 8,
        ),
        name="attend",
    )(queries, keys, values, asked, barred)


def attend_back_kernel(q_ref, k_ref, v_ref, g_ref, lse_ref, asked_ref, barred_ref, dq_ref, dk_ref, dv_ref, acc_k, acc_v):
    full = low_half((MB_TOK, LANES))
    tile_half = low_half((TILE, LANES))
    keys = k_ref[...]
    barred = barred_ref[...]
    values = v_ref[...]
    zero = jnp.zeros_like(values)
    keys_of = (jnp.where(full, keys, barred), jnp.where(full, barred, keys))
    values_of = (jnp.where(full, values, zero), jnp.where(full, zero, values))
    keys_turned = keys.astype(F32).T.astype(BF16)
    for step in range(MB_TOK // TILE):
        rows = pl.ds(step * TILE, TILE)
        queries = q_ref[rows, :]
        asked = asked_ref[rows, :]
        grads = g_ref[rows, :]
        turned = []
        for side in range(2):
            if side == 0:
                query = jnp.where(tile_half, queries, asked)
            else:
                query = jnp.where(tile_half, asked, queries)
            scores = contract_last(keys_of[side], query)
            probs = jnp.exp(scores - lse_ref[0, 0, 8 * side:8 * side + 1, rows])
            grad_probs = contract_last(values_of[side], grads)
            product = probs * grad_probs
            centre = jnp.sum(product, axis=0, keepdims=True)
            grad_scores = (product - probs * centre).astype(BF16)
            part_v = matmul(probs.astype(BF16), grads)
            part_k = matmul(grad_scores, queries)
            if step == 0:
                acc_v[side] = part_v
                acc_k[side] = part_k
            else:
                acc_v[side] += part_v
                acc_k[side] += part_k
            turned.append(matmul(keys_turned[side * HEAD_DIM:(side + 1) * HEAD_DIM, :], grad_scores))
        dq_ref[rows, :] = jnp.concatenate(turned, axis=0).T.astype(BF16)
    dk_ref[...] = jnp.where(full, acc_k[0], acc_k[1]).astype(BF16)
    dv_ref[...] = jnp.where(full, acc_v[0], acc_v[1]).astype(BF16)


def attend_back(queries, keys, values, grads, lse, asked, barred):
    rows = queries.shape[0]
    micro = rows // MB_TOK
    wide = pl.BlockSpec((MB_TOK, LANES), lambda m, p: (m, p))
    side = pl.BlockSpec((MB_TOK, LANES), lambda m, p: (m, 0))
    return pl.pallas_call(
        attend_back_kernel,
        grid=(micro, PAIRS),
        in_specs=[wide, wide, wide, wide, pl.BlockSpec((1, 1, 16, MB_TOK), lambda m, p: (m, p, 0, 0)), side, side],
        out_specs=[wide, wide, wide],
        out_shape=(jax.ShapeDtypeStruct(queries.shape, BF16),) * 3,
        scratch_shapes=[pltpu.VMEM((2, MB_TOK, LANES), F32), pltpu.VMEM((2, MB_TOK, LANES), F32)],
        compiler_params=pltpu.CompilerParams(vmem_limit_bytes=56 << 20),
        cost_estimate=pl.CostEstimate(
            flops=10 * rows * MB_TOK * HEADS * HEAD_DIM,
            transcendentals=rows * MB_TOK * HEADS,
            bytes_accessed=rows * 768 * 14,
        ),
        name="attend_back",
    )(queries, keys, values, grads, lse, asked, barred)


def norm_stats(value):
    center = value - jnp.mean(value, axis=-1, keepdims=True)
    spread = jnp.mean(center * center, axis=-1, keepdims=True)
    scale = lax.rsqrt(spread + EPSILON)
    return center * scale, scale


def norm_back(grad, normed, scale, gain):
    u = grad * gain
    return scale * (
        u
        - jnp.mean(u, axis=-1, keepdims=True)
        - normed * jnp.mean(u * normed, axis=-1, keepdims=True)
    )


def slot_positions(targets, rows_dev, slot_rows, device_count):
    owner_dev = targets // rows_dev
    chunks = rows_dev // BLOCK
    onehot = (owner_dev[:, None] == jnp.arange(device_count, dtype=jnp.int32)[None, :]).astype(BF16)
    onehot = onehot.reshape(chunks, BLOCK, device_count)
    steps = jnp.arange(BLOCK)
    earlier = (steps[:, None] > steps[None, :]).astype(BF16)
    inner = jnp.einsum("ij,cjd->cid", earlier, onehot, preferred_element_type=F32)
    sums = jnp.sum(onehot.astype(F32), axis=1)
    places = jnp.arange(chunks)
    outer = jnp.sum(jnp.where((places[:, None] > places[None, :])[:, :, None], sums[None], 0.0), axis=1)
    rank = jnp.sum((inner + outer[:, None, :]) * onehot.astype(F32), axis=2)
    return owner_dev * slot_rows + rank.reshape(rows_dev).astype(jnp.int32)


def invert(positions):
    return (
        jnp.zeros_like(positions).at[positions].set(jnp.arange(positions.shape[0], dtype=jnp.int32))
    )


def gather(value, tiled=True):
    return lax.all_gather(value, "dp", axis=0, tiled=tiled)


def scatter_sum(value):
    return lax.psum_scatter(value, "dp", scatter_dimension=0, tiled=False)


def exchange(rows, device_count):
    count, width = rows.shape
    slots = rows.reshape(device_count, count // device_count, width)
    slots = lax.all_to_all(slots, "dp", split_axis=0, concat_axis=0, tiled=True)
    return slots.reshape(count, width)


def layer_step(
    tokens,
    teacher,
    route_to,
    anchor,
    seq_lengths,
    query_weight,
    query_bias,
    key_weight,
    value_weight,
    value_bias,
    out_weight,
    out_bias,
    first_gain,
    first_shift,
    up_weight,
    up_bias,
    down_weight,
    down_bias,
    second_gain,
    second_shift,
):
    rows_dev, width = tokens.shape
    device_count = lax.axis_size("dp")
    slot_rows = rows_dev // device_count
    micro_count = rows_dev // MB_TOK
    asked, barred, usable = sequence_tables(seq_lengths, micro_count)

    count = jnp.sum(seq_lengths)
    pieces = jnp.stack([count // 64, count % 64]).astype(BF16)
    vectors = (query_bias, value_bias, out_bias, first_gain, first_shift, down_bias, second_gain, second_shift, up_bias)
    sizes = [v.shape[0] for v in vectors]
    used = sum(sizes) + 2
    extra = -(-used // width)
    packed = jnp.concatenate(list(vectors) + [pieces, jnp.zeros((extra * width - used,), BF16)])
    own = out_weight.shape[0]
    together = gather(
        jnp.concatenate([query_weight, key_weight, value_weight, out_weight, packed.reshape(extra, width)], axis=0),
        False,
    )
    w_q, w_k, w_v, w_out = (
        together[:, i * own:(i + 1) * own].reshape(device_count * own, width) for i in range(4)
    )
    gathered = together[:, 4 * own:].reshape(device_count, extra * width).astype(F32)
    w_up = gather(up_weight)
    w_down = gather(down_weight)
    full_vectors = []
    place = 0
    for size in sizes:
        full_vectors.append(gathered[:, place:place + size].reshape(-1))
        place += size
    q_b, v_b, o_b, g1, s1, d_b, g2, s2, u_b = full_vectors
    valid_count = jnp.sum(gathered[:, place] * 64.0 + gathered[:, place + 1])

    outgoing = slot_positions(route_to, rows_dev, slot_rows, device_count)
    incoming = slot_positions(anchor, rows_dev, slot_rows, device_count)
    send_order = invert(outgoing)
    back_order = invert(incoming)
    tokens_out, incoming, back_order = lax.optimization_barrier((tokens[send_order], incoming, back_order))
    x = exchange(tokens_out, device_count)[incoming]
    target = exchange(teacher[send_order], device_count)[incoming]

    queries = ((matmul(x, w_q) + q_b) * 0.125).astype(BF16)
    keys = matmul(x, w_k).astype(BF16)
    values = (matmul(x, w_v) + v_b).astype(BF16)
    attended, lse = attend(queries, keys, values, asked, barred)
    pre_first = x + (matmul(attended, w_out) + o_b)
    n1, r1 = norm_stats(pre_first)
    hidden = n1 * g1 + s1
    hidden_low = hidden.astype(BF16)
    pre_act = matmul(hidden_low, w_up) + u_b
    cdf = 0.5 * (1.0 + lax.erf(pre_act * (2.0 ** -0.5)))
    act_low = (pre_act * cdf).astype(BF16)
    slope = (cdf + pre_act * (jnp.exp(-0.5 * pre_act * pre_act) * 0.3989422804014327)).astype(BF16)
    pre_second = hidden + (matmul(act_low, w_down) + d_b)
    n2, r2 = norm_stats(pre_second)
    layer_out = n2 * g2 + s2
    misfit = jnp.where(usable[:, None], layer_out - target.astype(F32), 0.0)
    states_routed = layer_out.astype(BF16)
    squares = jnp.sum(misfit * misfit)
    states_out = states_routed[back_order]

    grad_out = misfit * (rows_dev * device_count * 2.0 / valid_count)
    grad_s2 = column_sum(grad_out)
    grad_g2 = column_sum(grad_out * n2)
    grad_pre_second = norm_back(grad_out, n2, r2, g2)
    down_grad, states_out = lax.optimization_barrier((grad_pre_second.astype(BF16), states_out))
    states = exchange(states_out, device_count)[outgoing]
    grad_w_down = cross_rows(act_low, down_grad).astype(BF16)
    grad_d_b = column_sum(down_grad)
    up_grad = (slope * contract_last(down_grad, w_down)).astype(BF16)
    grad_w_up = cross_rows(hidden_low, up_grad).astype(BF16)
    grad_u_b = column_sum(up_grad)
    up_own = up_weight.shape[0]
    down_own = down_weight.shape[0]
    chunks = up_weight.shape[1] // width
    blocks = [grad_w_down.reshape(device_count, down_own, width)] + [
        grad_w_up[:, c * width:(c + 1) * width].reshape(device_count, up_own, width) for c in range(chunks)
    ]
    up_grad, block = lax.optimization_barrier((up_grad, jnp.concatenate(blocks, axis=1)))
    share_ffn = scatter_sum(block)
    share_down = share_ffn[:down_own]
    share_up = jnp.concatenate(
        [share_ffn[down_own + c * up_own:down_own + (c + 1) * up_own] for c in range(chunks)], axis=1
    )
    back_up = contract_last(up_grad, w_up)
    grad_hidden = grad_pre_second + back_up
    grad_s1 = column_sum(grad_hidden)
    grad_g1 = column_sum(grad_hidden * n1)
    grad_pre_first = norm_back(grad_hidden, n1, r1, g1)
    out_grad = grad_pre_first.astype(BF16)
    grad_w_out = cross_rows(attended, out_grad).astype(BF16)
    grad_o_b = column_sum(out_grad)
    attended_grad = contract_last(out_grad, w_out).astype(BF16)
    dq, dk, dv = attend_back(queries, keys, values, attended_grad, lse, asked, barred)
    dq = dq * jnp.asarray(0.125, BF16)
    grad_q_b = column_sum(dq)
    grad_v_b = column_sum(dv)
    blocks = [cross_rows(x, dq).astype(BF16), cross_rows(x, dk).astype(BF16), cross_rows(x, dv).astype(BF16), grad_w_out]
    block = jnp.concatenate([g.reshape(device_count, own, width) for g in blocks], axis=1)
    dq, dk, dv, block = lax.optimization_barrier((dq, dk, dv, block))
    share_att = scatter_sum(block).astype(F32)
    rows_grad = (grad_pre_first + contract_last(dq, w_q) + contract_last(dk, w_k) + contract_last(dv, w_v)).astype(BF16)
    token_grad = exchange(rows_grad[back_order], device_count)[outgoing]
    grad_vectors = (grad_q_b, grad_v_b, grad_o_b, grad_g1, grad_s1, grad_d_b, grad_g2, grad_s2, grad_u_b)
    total_block = jnp.broadcast_to(squares.reshape(1, 1), (device_count, 1))
    grad_used = sum(sizes) + 1
    fill = jnp.zeros((device_count, -(-grad_used // 128) * 128 - grad_used), F32)
    grad_packed = jnp.concatenate(
        [g.reshape(device_count, -1) for g in grad_vectors] + [total_block, fill], axis=1
    )
    shares = lax.all_to_all(grad_packed, "dp", split_axis=0, concat_axis=0, tiled=True)
    summed = jnp.sum(shares, axis=0)
    parts = []
    place = 0
    for size in sizes:
        parts.append(summed[place:place + size])
        place += size
    h_q_b, h_v_b, h_o_b, h_g1, h_s1, h_d_b, h_g2, h_s2, h_u_b = parts
    mse_loss = summed[place] / valid_count
    return (
        states,
        mse_loss,
        token_grad,
        share_att[:own],
        h_q_b,
        share_att[own:2 * own],
        share_att[2 * own:3 * own],
        h_v_b,
        share_att[3 * own:],
        h_o_b,
        h_g1,
        h_s1,
        share_up.astype(F32),
        h_u_b,
        share_down.astype(F32),
        h_d_b,
        h_g2,
        h_s2,
    )


def solution(mesh):
    row = P("dp", None)
    vec = P("dp")
    placed = (row, row, vec, vec, vec, row, vec, row, row, vec, row, vec, vec, vec, row, vec, row, vec, vec, vec)
    return jax.shard_map(
        layer_step,
        mesh=mesh,
        in_specs=placed,
        out_specs=(row, P(), row, row, vec, row, row, vec, row, vec, vec, vec, row, vec, row, vec, vec, vec),
        check_vma=False,
    )
```

```python
import jax
import jax.numpy as jnp
from jax import lax
from jax.experimental import pallas as pl
from jax.experimental.pallas import tpu as pltpu
from jax.sharding import PartitionSpec as P


HEADS = 12
HEAD_DIM = 64
PAIRS = HEADS // 2
LANES = 2 * HEAD_DIM
BLOCK = 128
MB_TOK = 1024
SEQS = MB_TOK // BLOCK
TILE = 256
EPSILON = 1e-12
NEG = -1e30
F32 = jnp.float32
BF16 = jnp.bfloat16


def matmul(left, right):
    return jnp.dot(left, right, preferred_element_type=F32)


def contract_last(left, right):
    return lax.dot_general(left, right, (((1,), (1,)), ((), ())), preferred_element_type=F32)


def cross_rows(left, right):
    return lax.dot_general(left, right, (((0,), (0,)), ((), ())), preferred_element_type=F32)


def column_sum(value):
    return jnp.sum(value, axis=0, dtype=F32)


def sequence_tables(lengths_flat, groups):
    length_grid = lengths_flat.reshape(groups, SEQS)
    blocks = (length_grid + BLOCK - 1) // BLOCK
    before = jnp.arange(SEQS)[:, None] > jnp.arange(SEQS)[None, :]
    starts = jnp.sum(jnp.where(before[None], blocks[:, None, :], 0), axis=2)
    places = jnp.arange(MB_TOK, dtype=jnp.int32)[None, :, None]
    first = (starts * BLOCK)[:, None, :]
    member = (places >= first) & (places < ((starts + blocks) * BLOCK)[:, None, :])
    live = (places >= first) & (places < first + length_grid[:, None, :])
    usable = jnp.any(live, axis=2)
    pad = ((0, 0), (0, 0), (0, HEAD_DIM - SEQS))
    asked = jnp.pad(member.astype(BF16), pad)
    barred = jnp.pad(jnp.where(live, 0.0, NEG).astype(BF16), pad)
    asked = jnp.concatenate([asked, asked], axis=2)
    barred = jnp.concatenate([barred, barred], axis=2)
    rows = groups * MB_TOK
    return asked.reshape(rows, LANES), barred.reshape(rows, LANES), usable.reshape(rows)


def low_half(shape):
    return lax.broadcasted_iota(jnp.int32, shape, 1) < HEAD_DIM


def attend_kernel(q_ref, k_ref, v_ref, asked_ref, barred_ref, out_ref, lse_ref):
    full = low_half((MB_TOK, LANES))
    tile_half = low_half((TILE, LANES))
    ones = jnp.ones((MB_TOK, LANES), BF16)
    keys = k_ref[...]
    barred = barred_ref[...]
    values = v_ref[...]
    keys_of = (jnp.where(full, keys, barred), jnp.where(full, barred, keys))
    values_of = (jnp.where(full, values, ones), jnp.where(full, ones, values))
    for step in range(MB_TOK // TILE):
        rows = pl.ds(step * TILE, TILE)
        queries = q_ref[rows, :]
        asked = asked_ref[rows, :]
        outs = []
        logs = []
        for side in range(2):
            if side == 0:
                query = jnp.where(tile_half, queries, asked)
            else:
                query = jnp.where(tile_half, asked, queries)
            scores = contract_last(query, keys_of[side])
            peak = jnp.max(scores, axis=1, keepdims=True)
            probs = jnp.exp(scores - peak).astype(BF16)
            mixed = matmul(probs, values_of[side])
            total = pltpu.roll(mixed, HEAD_DIM, 1)
            outs.append(mixed / total)
            both = jnp.where(tile_half, total, mixed) if side == 0 else jnp.where(tile_half, mixed, total)
            logs.append(peak + jnp.log(both))
        out_ref[rows, :] = jnp.where(tile_half, outs[0], outs[1]).astype(BF16)
        logs = jnp.where(tile_half, logs[0], logs[1]).T
        lse_ref[0, 0, 0:8, rows] = logs[0:8, :]
        lse_ref[0, 0, 8:16, rows] = logs[HEAD_DIM:HEAD_DIM + 8, :]


def attend(queries, keys, values, asked, barred):
    rows = queries.shape[0]
    micro = rows // MB_TOK
    wide = pl.BlockSpec((MB_TOK, LANES), lambda m, p: (m, p))
    side = pl.BlockSpec((MB_TOK, LANES), lambda m, p: (m, 0))
    return pl.pallas_call(
        attend_kernel,
        grid=(micro, PAIRS),
        in_specs=[wide, wide, wide, side, side],
        out_specs=[wide, pl.BlockSpec((1, 1, 16, MB_TOK), lambda m, p: (m, p, 0, 0))],
        out_shape=(
            jax.ShapeDtypeStruct(queries.shape, BF16),
            jax.ShapeDtypeStruct((micro, PAIRS, 16, MB_TOK), F32),
        ),
        compiler_params=pltpu.CompilerParams(vmem_limit_bytes=56 << 20),
        cost_estimate=pl.CostEstimate(
            flops=4 * rows * MB_TOK * HEADS * HEAD_DIM,
            transcendentals=rows * MB_TOK * HEADS,
            bytes_accessed=rows * 768 * 8,
        ),
        name="attend",
    )(queries, keys, values, asked, barred)


def attend_back_kernel(q_ref, k_ref, v_ref, g_ref, lse_ref, asked_ref, barred_ref, dq_ref, dk_ref, dv_ref, acc_k, acc_v):
    full = low_half((MB_TOK, LANES))
    tile_half = low_half((TILE, LANES))
    keys = k_ref[...]
    barred = barred_ref[...]
    values = v_ref[...]
    zero = jnp.zeros_like(values)
    keys_of = (jnp.where(full, keys, barred), jnp.where(full, barred, keys))
    values_of = (jnp.where(full, values, zero), jnp.where(full, zero, values))
    keys_turned = keys.astype(F32).T.astype(BF16)
    for step in range(MB_TOK // TILE):
        rows = pl.ds(step * TILE, TILE)
        queries = q_ref[rows, :]
        asked = asked_ref[rows, :]
        grads = g_ref[rows, :]
        turned = []
        for side in range(2):
            if side == 0:
                query = jnp.where(tile_half, queries, asked)
            else:
                query = jnp.where(tile_half, asked, queries)
            scores = contract_last(keys_of[side], query)
            probs = jnp.exp(scores - lse_ref[0, 0, 8 * side:8 * side + 1, rows])
            grad_probs = contract_last(values_of[side], grads)
            product = probs * grad_probs
            centre = jnp.sum(product, axis=0, keepdims=True)
            grad_scores = (product - probs * centre).astype(BF16)
            part_v = matmul(probs.astype(BF16), grads)
            part_k = matmul(grad_scores, queries)
            if step == 0:
                acc_v[side] = part_v
                acc_k[side] = part_k
            else:
                acc_v[side] += part_v
                acc_k[side] += part_k
            turned.append(matmul(keys_turned[side * HEAD_DIM:(side + 1) * HEAD_DIM, :], grad_scores))
        dq_ref[rows, :] = jnp.concatenate(turned, axis=0).T.astype(BF16)
    dk_ref[...] = jnp.where(full, acc_k[0], acc_k[1]).astype(BF16)
    dv_ref[...] = jnp.where(full, acc_v[0], acc_v[1]).astype(BF16)


def attend_back(queries, keys, values, grads, lse, asked, barred):
    rows = queries.shape[0]
    micro = rows // MB_TOK
    wide = pl.BlockSpec((MB_TOK, LANES), lambda m, p: (m, p))
    side = pl.BlockSpec((MB_TOK, LANES), lambda m, p: (m, 0))
    return pl.pallas_call(
        attend_back_kernel,
        grid=(micro, PAIRS),
        in_specs=[wide, wide, wide, wide, pl.BlockSpec((1, 1, 16, MB_TOK), lambda m, p: (m, p, 0, 0)), side, side],
        out_specs=[wide, wide, wide],
        out_shape=(jax.ShapeDtypeStruct(queries.shape, BF16),) * 3,
        scratch_shapes=[pltpu.VMEM((2, MB_TOK, LANES), F32), pltpu.VMEM((2, MB_TOK, LANES), F32)],
        compiler_params=pltpu.CompilerParams(vmem_limit_bytes=56 << 20),
        cost_estimate=pl.CostEstimate(
            flops=10 * rows * MB_TOK * HEADS * HEAD_DIM,
            transcendentals=rows * MB_TOK * HEADS,
            bytes_accessed=rows * 768 * 14,
        ),
        name="attend_back",
    )(queries, keys, values, grads, lse, asked, barred)


def row_mean(value):
    return jnp.sum(value, axis=-1, keepdims=True) * (1.0 / value.shape[-1])


def middle_kernel(
    att_ref, x_ref, target_ref, usable_ref, w_out_ref, w_up_ref, w_down_ref, vec_ref, ub_ref,
    states_ref, hidden_ref, act_ref, down_ref, up_ref, first_ref, out_ref, attg_ref, sums_ref, ubsum_ref,
    slope_ref,
):
    width = x_ref.shape[1]
    chunks = w_up_ref.shape[1] // width
    o_b, g1, s1, d_b, g2, s2, scale = (vec_ref[i:i + 1, :] for i in range(7))

    @pl.when(pl.program_id(0) == 0)
    def _():
        sums_ref[...] = jnp.zeros_like(sums_ref)
        ubsum_ref[...] = jnp.zeros_like(ubsum_ref)

    pre_first = x_ref[...].astype(F32) + (matmul(att_ref[...], w_out_ref[...]) + o_b)
    center = pre_first - row_mean(pre_first)
    r1 = lax.rsqrt(row_mean(center * center) + EPSILON)
    n1 = center * r1
    hidden = n1 * g1 + s1
    hidden_low = hidden.astype(BF16)
    hidden_ref[...] = hidden_low
    total = hidden + d_b
    for c in range(chunks):
        cols = slice(c * width, (c + 1) * width)
        pre_act = matmul(hidden_low, w_up_ref[:, cols]) + ub_ref[0:1, cols]
        cdf = 0.5 * (1.0 + lax.erf(pre_act * (2.0 ** -0.5)))
        act_low = (pre_act * cdf).astype(BF16)
        slope = cdf + pre_act * (jnp.exp(-0.5 * pre_act * pre_act) * 0.3989422804014327)
        act_ref[:, cols] = act_low
        slope_ref[:, cols] = slope.astype(BF16)
        total += matmul(act_low, w_down_ref[cols, :])
    center = total - row_mean(total)
    r2 = lax.rsqrt(row_mean(center * center) + EPSILON)
    n2 = center * r2
    layer_out = n2 * g2 + s2
    states_ref[...] = layer_out.astype(BF16)
    misfit = jnp.where(usable_ref[...] > 0.5, layer_out - target_ref[...].astype(F32), 0.0)
    grad_out = misfit * scale
    u = grad_out * g2
    grad_second = r2 * (u - row_mean(u) - n2 * row_mean(u * n2))
    down_grad = grad_second.astype(BF16)
    down_ref[...] = down_grad
    sums_ref[0:1, :] += jnp.sum(grad_out, axis=0, keepdims=True)
    sums_ref[1:2, :] += jnp.sum(grad_out * n2, axis=0, keepdims=True)
    sums_ref[2:3, :] += jnp.sum(down_grad.astype(F32), axis=0, keepdims=True)
    sums_ref[6:7, :] += jnp.sum(misfit * misfit, axis=0, keepdims=True)
    grad_hidden = grad_second
    for c in range(chunks):
        cols = slice(c * width, (c + 1) * width)
        grad_act = contract_last(down_grad, w_down_ref[cols, :])
        up_grad = (slope_ref[:, cols].astype(F32) * grad_act).astype(BF16)
        up_ref[:, cols] = up_grad
        ubsum_ref[0:1, cols] += jnp.sum(up_grad.astype(F32), axis=0, keepdims=True)
        grad_hidden += contract_last(up_grad, w_up_ref[:, cols])
    u = grad_hidden * g1
    grad_first = r1 * (u - row_mean(u) - n1 * row_mean(u * n1))
    first_ref[...] = grad_first
    out_grad = grad_first.astype(BF16)
    out_ref[...] = out_grad
    sums_ref[3:4, :] += jnp.sum(grad_hidden, axis=0, keepdims=True)
    sums_ref[4:5, :] += jnp.sum(grad_hidden * n1, axis=0, keepdims=True)
    sums_ref[5:6, :] += jnp.sum(out_grad.astype(F32), axis=0, keepdims=True)
    attg_ref[...] = contract_last(out_grad, w_out_ref[...]).astype(BF16)


def middle(attended, x, target, usable, w_out, w_up, w_down, vectors, u_b):
    rows, width = x.shape
    wide = w_up.shape[1]
    row = pl.BlockSpec((TILE, width), lambda i: (i, 0))
    long = pl.BlockSpec((TILE, wide), lambda i: (i, 0))
    whole = lambda shape: pl.BlockSpec(shape, lambda i: (0, 0), pipeline_mode=pl.Buffered(1))
    still = lambda shape: pl.BlockSpec(shape, lambda i: (0, 0))
    shape = jax.ShapeDtypeStruct
    return pl.pallas_call(
        middle_kernel,
        grid=(rows // TILE,),
        in_specs=[
            row, row, row, pl.BlockSpec((TILE, 1), lambda i: (i, 0)),
            whole(w_out.shape), whole(w_up.shape), whole(w_down.shape), whole(vectors.shape), whole(u_b.shape),
        ],
        out_specs=[row, row, long, row, long, row, row, row, still((8, width)), still((8, wide))],
        out_shape=(
            shape((rows, width), BF16), shape((rows, width), BF16), shape((rows, wide), BF16),
            shape((rows, width), BF16), shape((rows, wide), BF16), shape((rows, width), F32),
            shape((rows, width), BF16), shape((rows, width), BF16), shape((8, width), F32), shape((8, wide), F32),
        ),
        scratch_shapes=[pltpu.VMEM((TILE, wide), BF16)],
        compiler_params=pltpu.CompilerParams(vmem_limit_bytes=58 << 20),
        cost_estimate=pl.CostEstimate(
            flops=2 * rows * width * (2 * width + 4 * wide),
            transcendentals=2 * rows * wide,
            bytes_accessed=rows * (width * 20 + wide * 4) + 4 * wide * width,
        ),
        name="middle",
    )(attended, x, target, usable, w_out, w_up, w_down, vectors, u_b)


def slot_positions(targets, rows_dev, slot_rows, device_count):
    owner_dev = targets // rows_dev
    chunks = rows_dev // BLOCK
    onehot = (owner_dev[:, None] == jnp.arange(device_count, dtype=jnp.int32)[None, :]).astype(BF16)
    onehot = onehot.reshape(chunks, BLOCK, device_count)
    steps = jnp.arange(BLOCK)
    earlier = (steps[:, None] > steps[None, :]).astype(BF16)
    inner = jnp.einsum("ij,cjd->cid", earlier, onehot, preferred_element_type=F32)
    sums = jnp.sum(onehot.astype(F32), axis=1)
    places = jnp.arange(chunks)
    outer = jnp.sum(jnp.where((places[:, None] > places[None, :])[:, :, None], sums[None], 0.0), axis=1)
    rank = jnp.sum((inner + outer[:, None, :]) * onehot.astype(F32), axis=2)
    return owner_dev * slot_rows + rank.reshape(rows_dev).astype(jnp.int32)


def invert(positions):
    return (
        jnp.zeros_like(positions).at[positions].set(jnp.arange(positions.shape[0], dtype=jnp.int32))
    )


def gather(value, tiled=True):
    return lax.all_gather(value, "dp", axis=0, tiled=tiled)


def scatter_sum(value):
    return lax.psum_scatter(value, "dp", scatter_dimension=0, tiled=False)


def exchange(rows, device_count):
    count, width = rows.shape
    slots = rows.reshape(device_count, count // device_count, width)
    slots = lax.all_to_all(slots, "dp", split_axis=0, concat_axis=0, tiled=True)
    return slots.reshape(count, width)


def layer_step(
    tokens,
    teacher,
    route_to,
    anchor,
    seq_lengths,
    query_weight,
    query_bias,
    key_weight,
    value_weight,
    value_bias,
    out_weight,
    out_bias,
    first_gain,
    first_shift,
    up_weight,
    up_bias,
    down_weight,
    down_bias,
    second_gain,
    second_shift,
):
    rows_dev, width = tokens.shape
    device_count = lax.axis_size("dp")
    slot_rows = rows_dev // device_count
    micro_count = rows_dev // MB_TOK
    asked, barred, usable = sequence_tables(seq_lengths, micro_count)

    count = jnp.sum(seq_lengths)
    pieces = jnp.stack([count // 64, count % 64]).astype(BF16)
    vectors = (query_bias, value_bias, out_bias, first_gain, first_shift, down_bias, second_gain, second_shift, up_bias)
    sizes = [v.shape[0] for v in vectors]
    used = sum(sizes) + 2
    extra = -(-used // width)
    packed = jnp.concatenate(list(vectors) + [pieces, jnp.zeros((extra * width - used,), BF16)])
    own = out_weight.shape[0]
    together = gather(
        jnp.concatenate([query_weight, key_weight, value_weight, out_weight, packed.reshape(extra, width)], axis=0),
        False,
    )
    w_q, w_k, w_v, w_out = (
        together[:, i * own:(i + 1) * own].reshape(device_count * own, width) for i in range(4)
    )
    gathered = together[:, 4 * own:].reshape(device_count, extra * width).astype(F32)
    w_up = gather(up_weight)
    w_down = gather(down_weight)
    full_vectors = []
    place = 0
    for size in sizes:
        full_vectors.append(gathered[:, place:place + size].reshape(-1))
        place += size
    q_b, v_b, o_b, g1, s1, d_b, g2, s2, u_b = full_vectors
    valid_count = jnp.sum(gathered[:, place] * 64.0 + gathered[:, place + 1])

    outgoing = slot_positions(route_to, rows_dev, slot_rows, device_count)
    incoming = slot_positions(anchor, rows_dev, slot_rows, device_count)
    send_order = invert(outgoing)
    back_order = invert(incoming)
    tokens_out, incoming, back_order = lax.optimization_barrier((tokens[send_order], incoming, back_order))
    x = exchange(tokens_out, device_count)[incoming]
    target = exchange(teacher[send_order], device_count)[incoming]

    queries = ((matmul(x, w_q) + q_b) * 0.125).astype(BF16)
    keys = matmul(x, w_k).astype(BF16)
    values = (matmul(x, w_v) + v_b).astype(BF16)
    attended, lse = attend(queries, keys, values, asked, barred)
    scale = rows_dev * device_count * 2.0 / valid_count
    vectors = jnp.stack([o_b, g1, s1, d_b, g2, s2, jnp.full((width,), scale, F32), jnp.zeros((width,), F32)])
    (
        states_routed, hidden_low, act_low, down_grad, up_grad, grad_pre_first, out_grad, attended_grad, sums, up_sums,
    ) = middle(attended, x, target, usable.astype(F32)[:, None], w_out, w_up, w_down, vectors, u_b[None])
    grad_s2, grad_g2, grad_d_b, grad_s1, grad_g1, grad_o_b = (sums[i] for i in range(6))
    squares = jnp.sum(sums[6])
    grad_u_b = up_sums[0]
    states_out = states_routed[back_order]
    states = exchange(states_out, device_count)[outgoing]
    grad_w_down = cross_rows(act_low, down_grad).astype(BF16)
    grad_w_up = cross_rows(hidden_low, up_grad).astype(BF16)
    up_own = up_weight.shape[0]
    down_own = down_weight.shape[0]
    chunks = up_weight.shape[1] // width
    blocks = [grad_w_down.reshape(device_count, down_own, width)] + [
        grad_w_up[:, c * width:(c + 1) * width].reshape(device_count, up_own, width) for c in range(chunks)
    ]
    attended_grad, block = lax.optimization_barrier((attended_grad, jnp.concatenate(blocks, axis=1)))
    share_ffn = scatter_sum(block)
    share_down = share_ffn[:down_own]
    share_up = jnp.concatenate(
        [share_ffn[down_own + c * up_own:down_own + (c + 1) * up_own] for c in range(chunks)], axis=1
    )
    grad_w_out = cross_rows(attended, out_grad).astype(BF16)
    dq, dk, dv = attend_back(queries, keys, values, attended_grad, lse, asked, barred)
    dq = dq * jnp.asarray(0.125, BF16)
    grad_q_b = column_sum(dq)
    grad_v_b = column_sum(dv)
    blocks = [cross_rows(x, dq).astype(BF16), cross_rows(x, dk).astype(BF16), cross_rows(x, dv).astype(BF16), grad_w_out]
    block = jnp.concatenate([g.reshape(device_count, own, width) for g in blocks], axis=1)
    dq, dk, dv, block = lax.optimization_barrier((dq, dk, dv, block))
    share_att = scatter_sum(block).astype(F32)
    rows_grad = (grad_pre_first + contract_last(dq, w_q) + contract_last(dk, w_k) + contract_last(dv, w_v)).astype(BF16)
    token_grad = exchange(rows_grad[back_order], device_count)[outgoing]
    grad_vectors = (grad_q_b, grad_v_b, grad_o_b, grad_g1, grad_s1, grad_d_b, grad_g2, grad_s2, grad_u_b)
    total_block = jnp.broadcast_to(squares.reshape(1, 1), (device_count, 1))
    grad_used = sum(sizes) + 1
    fill = jnp.zeros((device_count, -(-grad_used // 128) * 128 - grad_used), F32)
    grad_packed = jnp.concatenate(
        [g.reshape(device_count, -1) for g in grad_vectors] + [total_block, fill], axis=1
    )
    shares = lax.all_to_all(grad_packed, "dp", split_axis=0, concat_axis=0, tiled=True)
    summed = jnp.sum(shares, axis=0)
    parts = []
    place = 0
    for size in sizes:
        parts.append(summed[place:place + size])
        place += size
    h_q_b, h_v_b, h_o_b, h_g1, h_s1, h_d_b, h_g2, h_s2, h_u_b = parts
    mse_loss = summed[place] / valid_count
    return (
        states,
        mse_loss,
        token_grad,
        share_att[:own],
        h_q_b,
        share_att[own:2 * own],
        share_att[2 * own:3 * own],
        h_v_b,
        share_att[3 * own:],
        h_o_b,
        h_g1,
        h_s1,
        share_up.astype(F32),
        h_u_b,
        share_down.astype(F32),
        h_d_b,
        h_g2,
        h_s2,
    )


def solution(mesh):
    row = P("dp", None)
    vec = P("dp")
    placed = (row, row, vec, vec, vec, row, vec, row, row, vec, row, vec, vec, vec, row, vec, row, vec, vec, vec)
    return jax.shard_map(
        layer_step,
        mesh=mesh,
        in_specs=placed,
        out_specs=(row, P(), row, row, vec, row, row, vec, row, vec, vec, vec, row, vec, row, vec, vec, vec),
        check_vma=False,
    )
```

```python
import jax
import jax.numpy as jnp
from jax import lax
from jax.experimental import pallas as pl
from jax.experimental.pallas import tpu as pltpu
from jax.sharding import PartitionSpec as P


HEADS = 12
HEAD_DIM = 64
PAIRS = HEADS // 2
LANES = 2 * HEAD_DIM
BLOCK = 128
MB_TOK = 1024
SEQS = MB_TOK // BLOCK
TILE = 256
EPSILON = 1e-12
NEG = -1e30
F32 = jnp.float32
BF16 = jnp.bfloat16


def matmul(left, right):
    return jnp.dot(left, right, preferred_element_type=F32)


def contract_last(left, right):
    return lax.dot_general(left, right, (((1,), (1,)), ((), ())), preferred_element_type=F32)


def cross_rows(left, right):
    return lax.dot_general(left, right, (((0,), (0,)), ((), ())), preferred_element_type=F32)


def column_sum(value):
    return jnp.sum(value, axis=0, dtype=F32)


def sequence_tables(lengths_flat, groups):
    length_grid = lengths_flat.reshape(groups, SEQS)
    blocks = (length_grid + BLOCK - 1) // BLOCK
    before = jnp.arange(SEQS)[:, None] > jnp.arange(SEQS)[None, :]
    starts = jnp.sum(jnp.where(before[None], blocks[:, None, :], 0), axis=2)
    places = jnp.arange(MB_TOK, dtype=jnp.int32)[None, :, None]
    first = (starts * BLOCK)[:, None, :]
    member = (places >= first) & (places < ((starts + blocks) * BLOCK)[:, None, :])
    live = (places >= first) & (places < first + length_grid[:, None, :])
    usable = jnp.any(live, axis=2)
    pad = ((0, 0), (0, 0), (0, HEAD_DIM - SEQS))
    asked = jnp.pad(member.astype(BF16), pad)
    barred = jnp.pad(jnp.where(live, 0.0, NEG).astype(BF16), pad)
    asked = jnp.concatenate([asked, asked], axis=2)
    barred = jnp.concatenate([barred, barred], axis=2)
    rows = groups * MB_TOK
    return asked.reshape(rows, LANES), barred.reshape(rows, LANES), usable.reshape(rows)


def low_half(shape):
    return lax.broadcasted_iota(jnp.int32, shape, 1) < HEAD_DIM


def attend_kernel(q_ref, k_ref, v_ref, asked_ref, barred_ref, out_ref, lse_ref):
    full = low_half((MB_TOK, LANES))
    tile_half = low_half((TILE, LANES))
    ones = jnp.ones((MB_TOK, LANES), BF16)
    keys = k_ref[...]
    barred = barred_ref[...]
    values = v_ref[...]
    keys_of = (jnp.where(full, keys, barred), jnp.where(full, barred, keys))
    values_of = (jnp.where(full, values, ones), jnp.where(full, ones, values))
    for step in range(MB_TOK // TILE):
        rows = pl.ds(step * TILE, TILE)
        queries = q_ref[rows, :]
        asked = asked_ref[rows, :]
        outs = []
        logs = []
        for side in range(2):
            if side == 0:
                query = jnp.where(tile_half, queries, asked)
            else:
                query = jnp.where(tile_half, asked, queries)
            scores = contract_last(query, keys_of[side])
            peak = jnp.max(scores, axis=1, keepdims=True)
            probs = jnp.exp(scores - peak).astype(BF16)
            mixed = matmul(probs, values_of[side])
            total = pltpu.roll(mixed, HEAD_DIM, 1)
            outs.append(mixed / total)
            both = jnp.where(tile_half, total, mixed) if side == 0 else jnp.where(tile_half, mixed, total)
            logs.append(peak + jnp.log(both))
        out_ref[rows, :] = jnp.where(tile_half, outs[0], outs[1]).astype(BF16)
        logs = jnp.where(tile_half, logs[0], logs[1]).T
        lse_ref[0, 0, 0:8, rows] = logs[0:8, :]
        lse_ref[0, 0, 8:16, rows] = logs[HEAD_DIM:HEAD_DIM + 8, :]


def attend(queries, keys, values, asked, barred):
    rows = queries.shape[0]
    micro = rows // MB_TOK
    wide = pl.BlockSpec((MB_TOK, LANES), lambda m, p: (m, p))
    side = pl.BlockSpec((MB_TOK, LANES), lambda m, p: (m, 0))
    return pl.pallas_call(
        attend_kernel,
        grid=(micro, PAIRS),
        in_specs=[wide, wide, wide, side, side],
        out_specs=[wide, pl.BlockSpec((1, 1, 16, MB_TOK), lambda m, p: (m, p, 0, 0))],
        out_shape=(
            jax.ShapeDtypeStruct(queries.shape, BF16),
            jax.ShapeDtypeStruct((micro, PAIRS, 16, MB_TOK), F32),
        ),
        compiler_params=pltpu.CompilerParams(vmem_limit_bytes=56 << 20),
        cost_estimate=pl.CostEstimate(
            flops=4 * rows * MB_TOK * HEADS * HEAD_DIM,
            transcendentals=rows * MB_TOK * HEADS,
            bytes_accessed=rows * 768 * 8,
        ),
        name="attend",
    )(queries, keys, values, asked, barred)


def attend_back_kernel(q_ref, k_ref, v_ref, g_ref, lse_ref, asked_ref, barred_ref, dq_ref, dk_ref, dv_ref, acc_k, acc_v):
    full = low_half((MB_TOK, LANES))
    tile_half = low_half((TILE, LANES))
    keys = k_ref[...]
    barred = barred_ref[...]
    values = v_ref[...]
    zero = jnp.zeros_like(values)
    keys_of = (jnp.where(full, keys, barred), jnp.where(full, barred, keys))
    values_of = (jnp.where(full, values, zero), jnp.where(full, zero, values))
    keys_turned = keys.astype(F32).T.astype(BF16)
    for step in range(MB_TOK // TILE):
        rows = pl.ds(step * TILE, TILE)
        queries = q_ref[rows, :]
        asked = asked_ref[rows, :]
        grads = g_ref[rows, :]
        turned = []
        for side in range(2):
            if side == 0:
                query = jnp.where(tile_half, queries, asked)
            else:
                query = jnp.where(tile_half, asked, queries)
            scores = contract_last(keys_of[side], query)
            probs = jnp.exp(scores - lse_ref[0, 0, 8 * side:8 * side + 1, rows])
            grad_probs = contract_last(values_of[side], grads)
            product = probs * grad_probs
            centre = jnp.sum(product, axis=0, keepdims=True)
            grad_scores = (product - probs * centre).astype(BF16)
            part_v = matmul(probs.astype(BF16), grads)
            part_k = matmul(grad_scores, queries)
            if step == 0:
                acc_v[side] = part_v
                acc_k[side] = part_k
            else:
                acc_v[side] += part_v
                acc_k[side] += part_k
            turned.append(matmul(keys_turned[side * HEAD_DIM:(side + 1) * HEAD_DIM, :], grad_scores))
        dq_ref[rows, :] = jnp.concatenate(turned, axis=0).T.astype(BF16)
    dk_ref[...] = jnp.where(full, acc_k[0], acc_k[1]).astype(BF16)
    dv_ref[...] = jnp.where(full, acc_v[0], acc_v[1]).astype(BF16)


def attend_back(queries, keys, values, grads, lse, asked, barred):
    rows = queries.shape[0]
    micro = rows // MB_TOK
    wide = pl.BlockSpec((MB_TOK, LANES), lambda m, p: (m, p))
    side = pl.BlockSpec((MB_TOK, LANES), lambda m, p: (m, 0))
    return pl.pallas_call(
        attend_back_kernel,
        grid=(micro, PAIRS),
        in_specs=[wide, wide, wide, wide, pl.BlockSpec((1, 1, 16, MB_TOK), lambda m, p: (m, p, 0, 0)), side, side],
        out_specs=[wide, wide, wide],
        out_shape=(jax.ShapeDtypeStruct(queries.shape, BF16),) * 3,
        scratch_shapes=[pltpu.VMEM((2, MB_TOK, LANES), F32), pltpu.VMEM((2, MB_TOK, LANES), F32)],
        compiler_params=pltpu.CompilerParams(vmem_limit_bytes=56 << 20),
        cost_estimate=pl.CostEstimate(
            flops=10 * rows * MB_TOK * HEADS * HEAD_DIM,
            transcendentals=rows * MB_TOK * HEADS,
            bytes_accessed=rows * 768 * 14,
        ),
        name="attend_back",
    )(queries, keys, values, grads, lse, asked, barred)


def row_mean(value):
    return jnp.sum(value, axis=-1, keepdims=True) * (1.0 / value.shape[-1])


def middle_kernel(
    att_ref, x_ref, target_ref, usable_ref, w_out_ref, w_up_ref, w_down_ref, vec_ref, ub_ref,
    states_ref, hidden_ref, act_ref, down_ref, up_ref, first_ref, out_ref, attg_ref, sums_ref, ubsum_ref,
    slope_ref,
):
    width = x_ref.shape[1]
    chunks = w_up_ref.shape[1] // width
    o_b, g1, s1, d_b, g2, s2, scale = (vec_ref[i:i + 1, :] for i in range(7))

    @pl.when(pl.program_id(0) == 0)
    def _():
        sums_ref[...] = jnp.zeros_like(sums_ref)
        ubsum_ref[...] = jnp.zeros_like(ubsum_ref)

    pre_first = x_ref[...].astype(F32) + (matmul(att_ref[...], w_out_ref[...]) + o_b)
    center = pre_first - row_mean(pre_first)
    r1 = lax.rsqrt(row_mean(center * center) + EPSILON)
    n1 = center * r1
    hidden = n1 * g1 + s1
    hidden_low = hidden.astype(BF16)
    hidden_ref[...] = hidden_low
    total = hidden + d_b
    for c in range(chunks):
        cols = slice(c * width, (c + 1) * width)
        pre_act = matmul(hidden_low, w_up_ref[:, cols]) + ub_ref[0:1, cols]
        cdf = 0.5 * (1.0 + lax.erf(pre_act * (2.0 ** -0.5)))
        act_low = (pre_act * cdf).astype(BF16)
        slope = cdf + pre_act * (jnp.exp(-0.5 * pre_act * pre_act) * 0.3989422804014327)
        act_ref[:, cols] = act_low
        slope_ref[:, cols] = slope.astype(BF16)
        total += matmul(act_low, w_down_ref[cols, :])
    center = total - row_mean(total)
    r2 = lax.rsqrt(row_mean(center * center) + EPSILON)
    n2 = center * r2
    layer_out = n2 * g2 + s2
    states_ref[...] = layer_out.astype(BF16)
    misfit = jnp.where(usable_ref[...] > 0.5, layer_out - target_ref[...].astype(F32), 0.0)
    grad_out = misfit * scale
    u = grad_out * g2
    grad_second = r2 * (u - row_mean(u) - n2 * row_mean(u * n2))
    down_grad = grad_second.astype(BF16)
    down_ref[...] = down_grad
    sums_ref[0:1, :] += jnp.sum(grad_out, axis=0, keepdims=True)
    sums_ref[1:2, :] += jnp.sum(grad_out * n2, axis=0, keepdims=True)
    sums_ref[2:3, :] += jnp.sum(down_grad.astype(F32), axis=0, keepdims=True)
    sums_ref[6:7, :] += jnp.sum(misfit * misfit, axis=0, keepdims=True)
    grad_hidden = grad_second
    for c in range(chunks):
        cols = slice(c * width, (c + 1) * width)
        grad_act = contract_last(down_grad, w_down_ref[cols, :])
        up_grad = (slope_ref[:, cols].astype(F32) * grad_act).astype(BF16)
        up_ref[:, cols] = up_grad
        ubsum_ref[0:1, cols] += jnp.sum(up_grad.astype(F32), axis=0, keepdims=True)
        grad_hidden += contract_last(up_grad, w_up_ref[:, cols])
    u = grad_hidden * g1
    grad_first = r1 * (u - row_mean(u) - n1 * row_mean(u * n1))
    first_ref[...] = grad_first
    out_grad = grad_first.astype(BF16)
    out_ref[...] = out_grad
    sums_ref[3:4, :] += jnp.sum(grad_hidden, axis=0, keepdims=True)
    sums_ref[4:5, :] += jnp.sum(grad_hidden * n1, axis=0, keepdims=True)
    sums_ref[5:6, :] += jnp.sum(out_grad.astype(F32), axis=0, keepdims=True)
    attg_ref[...] = contract_last(out_grad, w_out_ref[...]).astype(BF16)


def middle(attended, x, target, usable, w_out, w_up, w_down, vectors, u_b):
    rows, width = x.shape
    wide = w_up.shape[1]
    row = pl.BlockSpec((TILE, width), lambda i: (i, 0))
    long = pl.BlockSpec((TILE, wide), lambda i: (i, 0))
    whole = lambda shape: pl.BlockSpec(shape, lambda i: (0, 0), pipeline_mode=pl.Buffered(1))
    still = lambda shape: pl.BlockSpec(shape, lambda i: (0, 0))
    shape = jax.ShapeDtypeStruct
    return pl.pallas_call(
        middle_kernel,
        grid=(rows // TILE,),
        in_specs=[
            row, row, row, pl.BlockSpec((TILE, 1), lambda i: (i, 0)),
            whole(w_out.shape), whole(w_up.shape), whole(w_down.shape), whole(vectors.shape), whole(u_b.shape),
        ],
        out_specs=[row, row, long, row, long, row, row, row, still((8, width)), still((8, wide))],
        out_shape=(
            shape((rows, width), BF16), shape((rows, width), BF16), shape((rows, wide), BF16),
            shape((rows, width), BF16), shape((rows, wide), BF16), shape((rows, width), F32),
            shape((rows, width), BF16), shape((rows, width), BF16), shape((8, width), F32), shape((8, wide), F32),
        ),
        scratch_shapes=[pltpu.VMEM((TILE, wide), BF16)],
        compiler_params=pltpu.CompilerParams(vmem_limit_bytes=58 << 20),
        cost_estimate=pl.CostEstimate(
            flops=2 * rows * width * (2 * width + 4 * wide),
            transcendentals=2 * rows * wide,
            bytes_accessed=rows * (width * 20 + wide * 4) + 4 * wide * width,
        ),
        name="middle",
    )(attended, x, target, usable, w_out, w_up, w_down, vectors, u_b)


def slot_positions(targets, rows_dev, slot_rows, device_count):
    owner_dev = targets // rows_dev
    chunks = rows_dev // BLOCK
    onehot = (owner_dev[:, None] == jnp.arange(device_count, dtype=jnp.int32)[None, :]).astype(BF16)
    onehot = onehot.reshape(chunks, BLOCK, device_count)
    steps = jnp.arange(BLOCK)
    earlier = (steps[:, None] > steps[None, :]).astype(BF16)
    inner = jnp.einsum("ij,cjd->cid", earlier, onehot, preferred_element_type=F32)
    sums = jnp.sum(onehot.astype(F32), axis=1)
    places = jnp.arange(chunks)
    outer = jnp.sum(jnp.where((places[:, None] > places[None, :])[:, :, None], sums[None], 0.0), axis=1)
    rank = jnp.sum((inner + outer[:, None, :]) * onehot.astype(F32), axis=2)
    return owner_dev * slot_rows + rank.reshape(rows_dev).astype(jnp.int32)


def place_kernel(pos_ref, rows_ref, out_ref):
    count = rows_ref.shape[0]
    first = pl.program_id(0) * TILE
    wanted = lax.broadcasted_iota(jnp.int32, (TILE, count), 0) + first
    chosen = jnp.where(wanted == pos_ref[0:1, :], 1.0, 0.0).astype(BF16)
    out_ref[...] = matmul(chosen, rows_ref[...]).astype(BF16)


def pick_kernel(pos_ref, rows_ref, out_ref):
    count = rows_ref.shape[0]
    column = jnp.broadcast_to(pos_ref[0:1, :].astype(F32), (BLOCK, TILE)).T[:, 0:1].astype(jnp.int32)
    chosen = jnp.where(lax.broadcasted_iota(jnp.int32, (TILE, count), 1) == column, 1.0, 0.0).astype(BF16)
    out_ref[...] = matmul(chosen, rows_ref[...]).astype(BF16)


def permute(positions, rows, pick):
    count, width = rows.shape
    if pick:
        pos_spec = pl.BlockSpec((1, TILE), lambda i: (0, i))
    else:
        pos_spec = pl.BlockSpec((1, count), lambda i: (0, 0))
    return pl.pallas_call(
        pick_kernel if pick else place_kernel,
        grid=(count // TILE,),
        in_specs=[pos_spec, pl.BlockSpec((count, width), lambda i: (0, 0), pipeline_mode=pl.Buffered(1))],
        out_specs=pl.BlockSpec((TILE, width), lambda i: (i, 0)),
        out_shape=jax.ShapeDtypeStruct((count, width), BF16),
        cost_estimate=pl.CostEstimate(
            flops=2 * count * count * width, transcendentals=0, bytes_accessed=4 * count * width
        ),
        name="pick" if pick else "place",
    )(positions.reshape(1, count), rows)


def gather(value, tiled=True):
    return lax.all_gather(value, "dp", axis=0, tiled=tiled)


def scatter_sum(value):
    return lax.psum_scatter(value, "dp", scatter_dimension=0, tiled=False)


def exchange(rows, device_count):
    count, width = rows.shape
    slots = rows.reshape(device_count, count // device_count, width)
    slots = lax.all_to_all(slots, "dp", split_axis=0, concat_axis=0, tiled=True)
    return slots.reshape(count, width)


def layer_step(
    tokens,
    teacher,
    route_to,
    anchor,
    seq_lengths,
    query_weight,
    query_bias,
    key_weight,
    value_weight,
    value_bias,
    out_weight,
    out_bias,
    first_gain,
    first_shift,
    up_weight,
    up_bias,
    down_weight,
    down_bias,
    second_gain,
    second_shift,
):
    rows_dev, width = tokens.shape
    device_count = lax.axis_size("dp")
    slot_rows = rows_dev // device_count
    micro_count = rows_dev // MB_TOK
    asked, barred, usable = sequence_tables(seq_lengths, micro_count)

    count = jnp.sum(seq_lengths)
    pieces = jnp.stack([count // 64, count % 64]).astype(BF16)
    vectors = (query_bias, value_bias, out_bias, first_gain, first_shift, down_bias, second_gain, second_shift, up_bias)
    sizes = [v.shape[0] for v in vectors]
    used = sum(sizes) + 2
    extra = -(-used // width)
    packed = jnp.concatenate(list(vectors) + [pieces, jnp.zeros((extra * width - used,), BF16)])
    own = out_weight.shape[0]
    together = gather(
        jnp.concatenate([query_weight, key_weight, value_weight, out_weight, packed.reshape(extra, width)], axis=0),
        False,
    )
    w_q, w_k, w_v, w_out = (
        together[:, i * own:(i + 1) * own].reshape(device_count * own, width) for i in range(4)
    )
    gathered = together[:, 4 * own:].reshape(device_count, extra * width).astype(F32)
    full_vectors = []
    place = 0
    for size in sizes:
        full_vectors.append(gathered[:, place:place + size].reshape(-1))
        place += size
    q_b, v_b, o_b, g1, s1, d_b, g2, s2, u_b = full_vectors
    valid_count = jnp.sum(gathered[:, place] * 64.0 + gathered[:, place + 1])
    up_own = up_weight.shape[0]
    down_own = down_weight.shape[0]
    chunks = up_weight.shape[1] // width
    ffn = gather(
        jnp.concatenate([down_weight] + [up_weight[:, c * width:(c + 1) * width] for c in range(chunks)], axis=0), False
    )
    w_down = ffn[:, :down_own].reshape(device_count * down_own, width)
    w_up = jnp.concatenate(
        [ffn[:, down_own + c * up_own:down_own + (c + 1) * up_own] for c in range(chunks)], axis=2
    ).reshape(device_count * up_own, chunks * width)

    outgoing = slot_positions(route_to, rows_dev, slot_rows, device_count)
    incoming = slot_positions(anchor, rows_dev, slot_rows, device_count)
    tokens_out, incoming = lax.optimization_barrier((permute(outgoing, tokens, False), incoming))
    x = permute(incoming, exchange(tokens_out, device_count), True)
    teacher_out = permute(outgoing, teacher, False)
    target = permute(incoming, exchange(teacher_out, device_count), True)

    queries = ((matmul(x, w_q) + q_b) * 0.125).astype(BF16)
    keys = matmul(x, w_k).astype(BF16)
    values = (matmul(x, w_v) + v_b).astype(BF16)
    attended, lse = attend(queries, keys, values, asked, barred)
    scale = rows_dev * device_count * 2.0 / valid_count
    vectors = jnp.stack([o_b, g1, s1, d_b, g2, s2, jnp.full((width,), scale, F32), jnp.zeros((width,), F32)])
    (
        states_routed, hidden_low, act_low, down_grad, up_grad, grad_pre_first, out_grad, attended_grad, sums, up_sums,
    ) = middle(attended, x, target, usable.astype(F32)[:, None], w_out, w_up, w_down, vectors, u_b[None])
    grad_s2, grad_g2, grad_d_b, grad_s1, grad_g1, grad_o_b = (sums[i] for i in range(6))
    squares = jnp.sum(sums[6])
    grad_u_b = up_sums[0]
    states = permute(outgoing, exchange(permute(incoming, states_routed, False), device_count), True)
    grad_w_down = cross_rows(act_low, down_grad).astype(BF16)
    grad_w_up = cross_rows(hidden_low, up_grad).astype(BF16)
    up_own = up_weight.shape[0]
    down_own = down_weight.shape[0]
    chunks = up_weight.shape[1] // width
    blocks = [grad_w_down.reshape(device_count, down_own, width)] + [
        grad_w_up[:, c * width:(c + 1) * width].reshape(device_count, up_own, width) for c in range(chunks)
    ]
    attended_grad, block = lax.optimization_barrier((attended_grad, jnp.concatenate(blocks, axis=1)))
    share_ffn = scatter_sum(block)
    share_down = share_ffn[:down_own]
    share_up = jnp.concatenate(
        [share_ffn[down_own + c * up_own:down_own + (c + 1) * up_own] for c in range(chunks)], axis=1
    )
    grad_w_out = cross_rows(attended, out_grad).astype(BF16)
    dq, dk, dv = attend_back(queries, keys, values, attended_grad, lse, asked, barred)
    dq = dq * jnp.asarray(0.125, BF16)
    grad_q_b = column_sum(dq)
    grad_v_b = column_sum(dv)
    blocks = [cross_rows(x, dq).astype(BF16), cross_rows(x, dk).astype(BF16), cross_rows(x, dv).astype(BF16), grad_w_out]
    block = jnp.concatenate([g.reshape(device_count, own, width) for g in blocks], axis=1)
    dq, dk, dv, block = lax.optimization_barrier((dq, dk, dv, block))
    share_att = scatter_sum(block).astype(F32)
    rows_grad = (grad_pre_first + contract_last(dq, w_q) + contract_last(dk, w_k) + contract_last(dv, w_v)).astype(BF16)
    token_grad = permute(outgoing, exchange(permute(incoming, rows_grad, False), device_count), True)
    grad_vectors = (grad_q_b, grad_v_b, grad_o_b, grad_g1, grad_s1, grad_d_b, grad_g2, grad_s2, grad_u_b)
    total_block = jnp.broadcast_to(squares.reshape(1, 1), (device_count, 1))
    grad_used = sum(sizes) + 1
    fill = jnp.zeros((device_count, -(-grad_used // 128) * 128 - grad_used), F32)
    grad_packed = jnp.concatenate(
        [g.reshape(device_count, -1) for g in grad_vectors] + [total_block, fill], axis=1
    )
    shares = lax.all_to_all(grad_packed, "dp", split_axis=0, concat_axis=0, tiled=True)
    summed = jnp.sum(shares, axis=0)
    parts = []
    place = 0
    for size in sizes:
        parts.append(summed[place:place + size])
        place += size
    h_q_b, h_v_b, h_o_b, h_g1, h_s1, h_d_b, h_g2, h_s2, h_u_b = parts
    mse_loss = summed[place] / valid_count
    return (
        states,
        mse_loss,
        token_grad,
        share_att[:own],
        h_q_b,
        share_att[own:2 * own],
        share_att[2 * own:3 * own],
        h_v_b,
        share_att[3 * own:],
        h_o_b,
        h_g1,
        h_s1,
        share_up.astype(F32),
        h_u_b,
        share_down.astype(F32),
        h_d_b,
        h_g2,
        h_s2,
    )


def solution(mesh):
    row = P("dp", None)
    vec = P("dp")
    placed = (row, row, vec, vec, vec, row, vec, row, row, vec, row, vec, vec, vec, row, vec, row, vec, vec, vec)
    return jax.shard_map(
        layer_step,
        mesh=mesh,
        in_specs=placed,
        out_specs=(row, P(), row, row, vec, row, row, vec, row, vec, vec, vec, row, vec, row, vec, vec, vec),
        check_vma=False,
    )
```

```python
import jax
import jax.numpy as jnp
from jax import lax
from jax.experimental import pallas as pl
from jax.experimental.pallas import tpu as pltpu
from jax.sharding import PartitionSpec as P


HEADS = 12
HEAD_DIM = 64
PAIRS = HEADS // 2
LANES = 2 * HEAD_DIM
BLOCK = 128
MB_TOK = 1024
SEQS = MB_TOK // BLOCK
TILE = 256
EPSILON = 1e-12
NEG = -1e30
F32 = jnp.float32
BF16 = jnp.bfloat16


def matmul(left, right):
    return jnp.dot(left, right, preferred_element_type=F32)


def contract_last(left, right):
    return lax.dot_general(left, right, (((1,), (1,)), ((), ())), preferred_element_type=F32)


def cross_rows(left, right):
    return lax.dot_general(left, right, (((0,), (0,)), ((), ())), preferred_element_type=F32)


def column_sum(value):
    return jnp.sum(value, axis=0, dtype=F32)


def sequence_tables(lengths_flat, groups):
    length_grid = lengths_flat.reshape(groups, SEQS)
    blocks = (length_grid + BLOCK - 1) // BLOCK
    before = jnp.arange(SEQS)[:, None] > jnp.arange(SEQS)[None, :]
    starts = jnp.sum(jnp.where(before[None], blocks[:, None, :], 0), axis=2)
    places = jnp.arange(MB_TOK, dtype=jnp.int32)[None, :, None]
    first = (starts * BLOCK)[:, None, :]
    member = (places >= first) & (places < ((starts + blocks) * BLOCK)[:, None, :])
    live = (places >= first) & (places < first + length_grid[:, None, :])
    usable = jnp.any(live, axis=2)
    pad = ((0, 0), (0, 0), (0, HEAD_DIM - SEQS))
    asked = jnp.pad(member.astype(BF16), pad)
    barred = jnp.pad(jnp.where(live, 0.0, NEG).astype(BF16), pad)
    asked = jnp.concatenate([asked, asked], axis=2)
    barred = jnp.concatenate([barred, barred], axis=2)
    rows = groups * MB_TOK
    return asked.reshape(rows, LANES), barred.reshape(rows, LANES), usable.reshape(rows)


def low_half(shape):
    return lax.broadcasted_iota(jnp.int32, shape, 1) < HEAD_DIM


def attend_kernel(q_ref, k_ref, v_ref, asked_ref, barred_ref, out_ref, lse_ref):
    full = low_half((MB_TOK, LANES))
    tile_half = low_half((TILE, LANES))
    ones = jnp.ones((MB_TOK, LANES), BF16)
    keys = k_ref[...]
    barred = barred_ref[...]
    values = v_ref[...]
    keys_of = (jnp.where(full, keys, barred), jnp.where(full, barred, keys))
    values_of = (jnp.where(full, values, ones), jnp.where(full, ones, values))
    for step in range(MB_TOK // TILE):
        rows = pl.ds(step * TILE, TILE)
        queries = q_ref[rows, :]
        asked = asked_ref[rows, :]
        outs = []
        logs = []
        for side in range(2):
            if side == 0:
                query = jnp.where(tile_half, queries, asked)
            else:
                query = jnp.where(tile_half, asked, queries)
            scores = contract_last(query, keys_of[side])
            peak = jnp.max(scores, axis=1, keepdims=True)
            probs = jnp.exp(scores - peak).astype(BF16)
            mixed = matmul(probs, values_of[side])
            total = pltpu.roll(mixed, HEAD_DIM, 1)
            outs.append(mixed / total)
            both = jnp.where(tile_half, total, mixed) if side == 0 else jnp.where(tile_half, mixed, total)
            logs.append(peak + jnp.log(both))
        out_ref[rows, :] = jnp.where(tile_half, outs[0], outs[1]).astype(BF16)
        logs = jnp.where(tile_half, logs[0], logs[1]).T
        lse_ref[0, 0, 0:8, rows] = logs[0:8, :]
        lse_ref[0, 0, 8:16, rows] = logs[HEAD_DIM:HEAD_DIM + 8, :]


def attend(queries, keys, values, asked, barred):
    rows = queries.shape[0]
    micro = rows // MB_TOK
    wide = pl.BlockSpec((MB_TOK, LANES), lambda m, p: (m, p))
    side = pl.BlockSpec((MB_TOK, LANES), lambda m, p: (m, 0))
    return pl.pallas_call(
        attend_kernel,
        grid=(micro, PAIRS),
        in_specs=[wide, wide, wide, side, side],
        out_specs=[wide, pl.BlockSpec((1, 1, 16, MB_TOK), lambda m, p: (m, p, 0, 0))],
        out_shape=(
            jax.ShapeDtypeStruct(queries.shape, BF16),
            jax.ShapeDtypeStruct((micro, PAIRS, 16, MB_TOK), F32),
        ),
        compiler_params=pltpu.CompilerParams(vmem_limit_bytes=56 << 20),
        cost_estimate=pl.CostEstimate(
            flops=4 * rows * MB_TOK * HEADS * HEAD_DIM,
            transcendentals=rows * MB_TOK * HEADS,
            bytes_accessed=rows * 768 * 8,
        ),
        name="attend",
    )(queries, keys, values, asked, barred)


def attend_back_kernel(q_ref, k_ref, v_ref, g_ref, lse_ref, asked_ref, barred_ref, dq_ref, dk_ref, dv_ref, acc_k, acc_v):
    full = low_half((MB_TOK, LANES))
    tile_half = low_half((TILE, LANES))
    keys = k_ref[...]
    barred = barred_ref[...]
    values = v_ref[...]
    zero = jnp.zeros_like(values)
    keys_of = (jnp.where(full, keys, barred), jnp.where(full, barred, keys))
    values_of = (jnp.where(full, values, zero), jnp.where(full, zero, values))
    keys_turned = keys.astype(F32).T.astype(BF16)
    for step in range(MB_TOK // TILE):
        rows = pl.ds(step * TILE, TILE)
        queries = q_ref[rows, :]
        asked = asked_ref[rows, :]
        grads = g_ref[rows, :]
        turned = []
        for side in range(2):
            if side == 0:
                query = jnp.where(tile_half, queries, asked)
            else:
                query = jnp.where(tile_half, asked, queries)
            scores = contract_last(keys_of[side], query)
            probs = jnp.exp(scores - lse_ref[0, 0, 8 * side:8 * side + 1, rows])
            grad_probs = contract_last(values_of[side], grads)
            product = probs * grad_probs
            centre = jnp.sum(product, axis=0, keepdims=True)
            grad_scores = (product - probs * centre).astype(BF16)
            part_v = matmul(probs.astype(BF16), grads)
            part_k = matmul(grad_scores, queries)
            if step == 0:
                acc_v[side] = part_v
                acc_k[side] = part_k
            else:
                acc_v[side] += part_v
                acc_k[side] += part_k
            turned.append(matmul(keys_turned[side * HEAD_DIM:(side + 1) * HEAD_DIM, :], grad_scores))
        dq_ref[rows, :] = jnp.concatenate(turned, axis=0).T.astype(BF16)
    dk_ref[...] = jnp.where(full, acc_k[0], acc_k[1]).astype(BF16)
    dv_ref[...] = jnp.where(full, acc_v[0], acc_v[1]).astype(BF16)


def attend_back(queries, keys, values, grads, lse, asked, barred):
    rows = queries.shape[0]
    micro = rows // MB_TOK
    wide = pl.BlockSpec((MB_TOK, LANES), lambda m, p: (m, p))
    side = pl.BlockSpec((MB_TOK, LANES), lambda m, p: (m, 0))
    return pl.pallas_call(
        attend_back_kernel,
        grid=(micro, PAIRS),
        in_specs=[wide, wide, wide, wide, pl.BlockSpec((1, 1, 16, MB_TOK), lambda m, p: (m, p, 0, 0)), side, side],
        out_specs=[wide, wide, wide],
        out_shape=(jax.ShapeDtypeStruct(queries.shape, BF16),) * 3,
        scratch_shapes=[pltpu.VMEM((2, MB_TOK, LANES), F32), pltpu.VMEM((2, MB_TOK, LANES), F32)],
        compiler_params=pltpu.CompilerParams(vmem_limit_bytes=56 << 20),
        cost_estimate=pl.CostEstimate(
            flops=10 * rows * MB_TOK * HEADS * HEAD_DIM,
            transcendentals=rows * MB_TOK * HEADS,
            bytes_accessed=rows * 768 * 14,
        ),
        name="attend_back",
    )(queries, keys, values, grads, lse, asked, barred)


def row_mean(value):
    return jnp.sum(value, axis=-1, keepdims=True) * (1.0 / value.shape[-1])


def ahead_kernel(
    att_ref, x_ref, w_out_ref, w_up_ref, w_down_ref, vec_ref, ub_ref,
    states_ref, hidden_ref, act_ref, slope_ref, n1_ref, r1_ref, n2_ref, r2_ref,
):
    width = x_ref.shape[1]
    chunks = w_up_ref.shape[1] // width
    o_b, g1, s1, d_b, g2, s2 = (vec_ref[i:i + 1, :] for i in range(6))
    pre_first = x_ref[...].astype(F32) + (matmul(att_ref[...], w_out_ref[...]) + o_b)
    center = pre_first - row_mean(pre_first)
    r1 = lax.rsqrt(row_mean(center * center) + EPSILON)
    n1 = center * r1
    r1_ref[...] = r1
    n1_ref[...] = n1
    hidden = n1 * g1 + s1
    hidden_low = hidden.astype(BF16)
    hidden_ref[...] = hidden_low
    total = hidden + d_b
    for c in range(chunks):
        cols = slice(c * width, (c + 1) * width)
        pre_act = matmul(hidden_low, w_up_ref[:, cols]) + ub_ref[0:1, cols]
        cdf = 0.5 * (1.0 + lax.erf(pre_act * (2.0 ** -0.5)))
        act_low = (pre_act * cdf).astype(BF16)
        slope = cdf + pre_act * (jnp.exp(-0.5 * pre_act * pre_act) * 0.3989422804014327)
        act_ref[:, cols] = act_low
        slope_ref[:, cols] = slope.astype(BF16)
        total += matmul(act_low, w_down_ref[cols, :])
    center = total - row_mean(total)
    r2 = lax.rsqrt(row_mean(center * center) + EPSILON)
    n2 = center * r2
    r2_ref[...] = r2
    n2_ref[...] = n2
    states_ref[...] = (n2 * g2 + s2).astype(BF16)


def return_kernel(
    target_ref, usable_ref, slope_ref, n1_ref, r1_ref, n2_ref, r2_ref, w_out_ref, w_up_ref, w_down_ref, vec_ref,
    down_ref, up_ref, first_ref, out_ref, attg_ref, sums_ref, ubsum_ref,
):
    width = target_ref.shape[1]
    chunks = w_up_ref.shape[1] // width
    _, g1, _, _, g2, s2, scale = (vec_ref[i:i + 1, :] for i in range(7))

    @pl.when(pl.program_id(0) == 0)
    def _():
        sums_ref[...] = jnp.zeros_like(sums_ref)
        ubsum_ref[...] = jnp.zeros_like(ubsum_ref)

    n1, r1, n2, r2 = n1_ref[...], r1_ref[...], n2_ref[...], r2_ref[...]
    misfit = jnp.where(usable_ref[...] > 0.5, n2 * g2 + s2 - target_ref[...].astype(F32), 0.0)
    grad_out = misfit * scale
    u = grad_out * g2
    grad_second = r2 * (u - row_mean(u) - n2 * row_mean(u * n2))
    down_grad = grad_second.astype(BF16)
    down_ref[...] = down_grad
    sums_ref[0:1, :] += jnp.sum(grad_out, axis=0, keepdims=True)
    sums_ref[1:2, :] += jnp.sum(grad_out * n2, axis=0, keepdims=True)
    sums_ref[2:3, :] += jnp.sum(down_grad.astype(F32), axis=0, keepdims=True)
    sums_ref[6:7, :] += jnp.sum(misfit * misfit, axis=0, keepdims=True)
    grad_hidden = grad_second
    for c in range(chunks):
        cols = slice(c * width, (c + 1) * width)
        grad_act = contract_last(down_grad, w_down_ref[cols, :])
        up_grad = (slope_ref[:, cols].astype(F32) * grad_act).astype(BF16)
        up_ref[:, cols] = up_grad
        ubsum_ref[0:1, cols] += jnp.sum(up_grad.astype(F32), axis=0, keepdims=True)
        grad_hidden += contract_last(up_grad, w_up_ref[:, cols])
    u = grad_hidden * g1
    grad_first = r1 * (u - row_mean(u) - n1 * row_mean(u * n1))
    first_ref[...] = grad_first
    out_grad = grad_first.astype(BF16)
    out_ref[...] = out_grad
    sums_ref[3:4, :] += jnp.sum(grad_hidden, axis=0, keepdims=True)
    sums_ref[4:5, :] += jnp.sum(grad_hidden * n1, axis=0, keepdims=True)
    sums_ref[5:6, :] += jnp.sum(out_grad.astype(F32), axis=0, keepdims=True)
    attg_ref[...] = contract_last(out_grad, w_out_ref[...]).astype(BF16)


def row_specs(width, wide):
    row = pl.BlockSpec((TILE, width), lambda i: (i, 0))
    long = pl.BlockSpec((TILE, wide), lambda i: (i, 0))
    thin = pl.BlockSpec((TILE, 1), lambda i: (i, 0))
    whole = lambda array: pl.BlockSpec(array.shape, lambda i: (0, 0), pipeline_mode=pl.Buffered(1))
    return row, long, thin, whole


def middle_ahead(attended, x, w_out, w_up, w_down, vectors, u_b):
    rows, width = x.shape
    wide = w_up.shape[1]
    row, long, thin, whole = row_specs(width, wide)
    shape = jax.ShapeDtypeStruct
    return pl.pallas_call(
        ahead_kernel,
        grid=(rows // TILE,),
        in_specs=[row, row, whole(w_out), whole(w_up), whole(w_down), whole(vectors), whole(u_b)],
        out_specs=[row, row, long, long, row, thin, row, thin],
        out_shape=(
            shape((rows, width), BF16), shape((rows, width), BF16), shape((rows, wide), BF16),
            shape((rows, wide), BF16), shape((rows, width), F32), shape((rows, 1), F32),
            shape((rows, width), F32), shape((rows, 1), F32),
        ),
        compiler_params=pltpu.CompilerParams(vmem_limit_bytes=58 << 20),
        cost_estimate=pl.CostEstimate(
            flops=2 * rows * width * (width + 2 * wide),
            transcendentals=2 * rows * wide,
            bytes_accessed=rows * (width * 16 + wide * 4) + 4 * wide * width,
        ),
        name="middle_ahead",
    )(attended, x, w_out, w_up, w_down, vectors, u_b)


def middle_back(target, usable, slope, n1, r1, n2, r2, w_out, w_up, w_down, vectors):
    rows, width = target.shape
    wide = w_up.shape[1]
    row, long, thin, whole = row_specs(width, wide)
    still = lambda dims: pl.BlockSpec(dims, lambda i: (0, 0))
    shape = jax.ShapeDtypeStruct
    return pl.pallas_call(
        return_kernel,
        grid=(rows // TILE,),
        in_specs=[row, thin, long, row, thin, row, thin, whole(w_out), whole(w_up), whole(w_down), whole(vectors)],
        out_specs=[row, long, row, row, row, still((8, width)), still((8, wide))],
        out_shape=(
            shape((rows, width), BF16), shape((rows, wide), BF16), shape((rows, width), F32),
            shape((rows, width), BF16), shape((rows, width), BF16), shape((8, width), F32), shape((8, wide), F32),
        ),
        compiler_params=pltpu.CompilerParams(vmem_limit_bytes=58 << 20),
        cost_estimate=pl.CostEstimate(
            flops=2 * rows * width * (width + 2 * wide),
            transcendentals=0,
            bytes_accessed=rows * (width * 20 + wide * 4) + 4 * wide * width,
        ),
        name="middle_back",
    )(target, usable, slope, n1, r1, n2, r2, w_out, w_up, w_down, vectors)


def slot_positions(targets, rows_dev, slot_rows, device_count):
    owner_dev = targets // rows_dev
    chunks = rows_dev // BLOCK
    onehot = (owner_dev[:, None] == jnp.arange(device_count, dtype=jnp.int32)[None, :]).astype(BF16)
    onehot = onehot.reshape(chunks, BLOCK, device_count)
    steps = jnp.arange(BLOCK)
    earlier = (steps[:, None] > steps[None, :]).astype(BF16)
    inner = jnp.einsum("ij,cjd->cid", earlier, onehot, preferred_element_type=F32)
    sums = jnp.sum(onehot.astype(F32), axis=1)
    places = jnp.arange(chunks)
    outer = jnp.sum(jnp.where((places[:, None] > places[None, :])[:, :, None], sums[None], 0.0), axis=1)
    rank = jnp.sum((inner + outer[:, None, :]) * onehot.astype(F32), axis=2)
    return owner_dev * slot_rows + rank.reshape(rows_dev).astype(jnp.int32)


def place_kernel(pos_ref, rows_ref, out_ref):
    count = rows_ref.shape[0]
    first = pl.program_id(0) * TILE
    wanted = lax.broadcasted_iota(jnp.int32, (TILE, count), 0) + first
    chosen = jnp.where(wanted == pos_ref[0:1, :], 1.0, 0.0).astype(BF16)
    out_ref[...] = matmul(chosen, rows_ref[...]).astype(BF16)


def pick_kernel(pos_ref, rows_ref, out_ref):
    count = rows_ref.shape[0]
    column = jnp.broadcast_to(pos_ref[0:1, :].astype(F32), (BLOCK, TILE)).T[:, 0:1].astype(jnp.int32)
    chosen = jnp.where(lax.broadcasted_iota(jnp.int32, (TILE, count), 1) == column, 1.0, 0.0).astype(BF16)
    out_ref[...] = matmul(chosen, rows_ref[...]).astype(BF16)


def permute(positions, rows, pick):
    count, width = rows.shape
    if pick:
        pos_spec = pl.BlockSpec((1, TILE), lambda i: (0, i))
    else:
        pos_spec = pl.BlockSpec((1, count), lambda i: (0, 0))
    return pl.pallas_call(
        pick_kernel if pick else place_kernel,
        grid=(count // TILE,),
        in_specs=[pos_spec, pl.BlockSpec((count, width), lambda i: (0, 0), pipeline_mode=pl.Buffered(1))],
        out_specs=pl.BlockSpec((TILE, width), lambda i: (i, 0)),
        out_shape=jax.ShapeDtypeStruct((count, width), BF16),
        cost_estimate=pl.CostEstimate(
            flops=2 * count * count * width, transcendentals=0, bytes_accessed=4 * count * width
        ),
        name="pick" if pick else "place",
    )(positions.reshape(1, count), rows)


def gather(value, tiled=True):
    return lax.all_gather(value, "dp", axis=0, tiled=tiled)


def scatter_sum(value):
    return lax.psum_scatter(value, "dp", scatter_dimension=0, tiled=False)


def exchange(rows, device_count):
    count, width = rows.shape
    slots = rows.reshape(device_count, count // device_count, width)
    slots = lax.all_to_all(slots, "dp", split_axis=0, concat_axis=0, tiled=True)
    return slots.reshape(count, width)


def layer_step(
    tokens,
    teacher,
    route_to,
    anchor,
    seq_lengths,
    query_weight,
    query_bias,
    key_weight,
    value_weight,
    value_bias,
    out_weight,
    out_bias,
    first_gain,
    first_shift,
    up_weight,
    up_bias,
    down_weight,
    down_bias,
    second_gain,
    second_shift,
):
    rows_dev, width = tokens.shape
    device_count = lax.axis_size("dp")
    slot_rows = rows_dev // device_count
    micro_count = rows_dev // MB_TOK
    asked, barred, usable = sequence_tables(seq_lengths, micro_count)

    count = jnp.sum(seq_lengths)
    pieces = jnp.stack([count // 64, count % 64]).astype(BF16)
    vectors = (query_bias, value_bias, out_bias, first_gain, first_shift, down_bias, second_gain, second_shift, up_bias)
    sizes = [v.shape[0] for v in vectors]
    used = sum(sizes) + 2
    extra = -(-used // width)
    packed = jnp.concatenate(list(vectors) + [pieces, jnp.zeros((extra * width - used,), BF16)])
    own = out_weight.shape[0]
    together = gather(
        jnp.concatenate([query_weight, key_weight, value_weight, out_weight, packed.reshape(extra, width)], axis=0),
        False,
    )
    w_q, w_k, w_v, w_out = (
        together[:, i * own:(i + 1) * own].reshape(device_count * own, width) for i in range(4)
    )
    gathered = together[:, 4 * own:].reshape(device_count, extra * width).astype(F32)
    full_vectors = []
    place = 0
    for size in sizes:
        full_vectors.append(gathered[:, place:place + size].reshape(-1))
        place += size
    q_b, v_b, o_b, g1, s1, d_b, g2, s2, u_b = full_vectors
    valid_count = jnp.sum(gathered[:, place] * 64.0 + gathered[:, place + 1])
    up_own = up_weight.shape[0]
    down_own = down_weight.shape[0]
    chunks = up_weight.shape[1] // width
    ffn = gather(
        jnp.concatenate([down_weight] + [up_weight[:, c * width:(c + 1) * width] for c in range(chunks)], axis=0), False
    )
    w_down = ffn[:, :down_own].reshape(device_count * down_own, width)
    w_up = jnp.concatenate(
        [ffn[:, down_own + c * up_own:down_own + (c + 1) * up_own] for c in range(chunks)], axis=2
    ).reshape(device_count * up_own, chunks * width)

    outgoing = slot_positions(route_to, rows_dev, slot_rows, device_count)
    incoming = slot_positions(anchor, rows_dev, slot_rows, device_count)
    tokens_out, incoming = lax.optimization_barrier((permute(outgoing, tokens, False), incoming))
    x = permute(incoming, exchange(tokens_out, device_count), True)
    teacher_out = permute(outgoing, teacher, False)
    target = permute(incoming, exchange(teacher_out, device_count), True)

    queries = ((matmul(x, w_q) + q_b) * 0.125).astype(BF16)
    keys = matmul(x, w_k).astype(BF16)
    values = (matmul(x, w_v) + v_b).astype(BF16)
    attended, lse = attend(queries, keys, values, asked, barred)
    scale = rows_dev * device_count * 2.0 / valid_count
    vectors = jnp.stack([o_b, g1, s1, d_b, g2, s2, jnp.full((width,), scale, F32), jnp.zeros((width,), F32)])
    states_routed, hidden_low, act_low, slope, n1, r1, n2, r2 = middle_ahead(
        attended, x, w_out, w_up, w_down, vectors, u_b[None]
    )
    down_grad, up_grad, grad_pre_first, out_grad, attended_grad, sums, up_sums = middle_back(
        target, usable.astype(F32)[:, None], slope, n1, r1, n2, r2, w_out, w_up, w_down, vectors
    )
    grad_s2, grad_g2, grad_d_b, grad_s1, grad_g1, grad_o_b = (sums[i] for i in range(6))
    squares = jnp.sum(sums[6])
    grad_u_b = up_sums[0]
    states = permute(outgoing, exchange(permute(incoming, states_routed, False), device_count), True)
    grad_w_down = cross_rows(act_low, down_grad).astype(BF16)
    grad_w_up = cross_rows(hidden_low, up_grad).astype(BF16)
    up_own = up_weight.shape[0]
    down_own = down_weight.shape[0]
    chunks = up_weight.shape[1] // width
    blocks = [grad_w_down.reshape(device_count, down_own, width)] + [
        grad_w_up[:, c * width:(c + 1) * width].reshape(device_count, up_own, width) for c in range(chunks)
    ]
    attended_grad, block = lax.optimization_barrier((attended_grad, jnp.concatenate(blocks, axis=1)))
    share_ffn = scatter_sum(block)
    share_down = share_ffn[:down_own]
    share_up = jnp.concatenate(
        [share_ffn[down_own + c * up_own:down_own + (c + 1) * up_own] for c in range(chunks)], axis=1
    )
    grad_w_out = cross_rows(attended, out_grad).astype(BF16)
    dq, dk, dv = attend_back(queries, keys, values, attended_grad, lse, asked, barred)
    dq = dq * jnp.asarray(0.125, BF16)
    grad_q_b = column_sum(dq)
    grad_v_b = column_sum(dv)
    blocks = [cross_rows(x, grad).astype(BF16) for grad in (dq, dk, dv)] + [grad_w_out]
    block = jnp.concatenate([g.reshape(device_count, own, width) for g in blocks], axis=1)
    share_att = scatter_sum(block).astype(F32)
    rows_grad = (grad_pre_first + contract_last(dq, w_q) + contract_last(dk, w_k) + contract_last(dv, w_v)).astype(BF16)
    token_grad = permute(outgoing, exchange(permute(incoming, rows_grad, False), device_count), True)
    grad_vectors = (grad_q_b, grad_v_b, grad_o_b, grad_g1, grad_s1, grad_d_b, grad_g2, grad_s2, grad_u_b)
    total_block = jnp.broadcast_to(squares.reshape(1, 1), (device_count, 1))
    grad_used = sum(sizes) + 1
    fill = jnp.zeros((device_count, -(-grad_used // 128) * 128 - grad_used), F32)
    grad_packed = jnp.concatenate(
        [g.reshape(device_count, -1) for g in grad_vectors] + [total_block, fill], axis=1
    )
    shares = lax.all_to_all(grad_packed, "dp", split_axis=0, concat_axis=0, tiled=True)
    summed = jnp.sum(shares, axis=0)
    parts = []
    place = 0
    for size in sizes:
        parts.append(summed[place:place + size])
        place += size
    h_q_b, h_v_b, h_o_b, h_g1, h_s1, h_d_b, h_g2, h_s2, h_u_b = parts
    mse_loss = summed[place] / valid_count
    return (
        states,
        mse_loss,
        token_grad,
        share_att[:own],
        h_q_b,
        share_att[own:2 * own],
        share_att[2 * own:3 * own],
        h_v_b,
        share_att[3 * own:],
        h_o_b,
        h_g1,
        h_s1,
        share_up.astype(F32),
        h_u_b,
        share_down.astype(F32),
        h_d_b,
        h_g2,
        h_s2,
    )


def solution(mesh):
    row = P("dp", None)
    vec = P("dp")
    placed = (row, row, vec, vec, vec, row, vec, row, row, vec, row, vec, vec, vec, row, vec, row, vec, vec, vec)
    return jax.shard_map(
        layer_step,
        mesh=mesh,
        in_specs=placed,
        out_specs=(row, P(), row, row, vec, row, row, vec, row, vec, vec, vec, row, vec, row, vec, vec, vec),
        check_vma=False,
    )
```
